32 devices in a mesh: seq: 8 (over z, x), mp: 4 (over y, core).
Axes of the slice: x: 2, y: 2, z: 4, core: 2. Of those that a mesh axis runs over, the one named last changes fastest.
Arguments:
- grad_rows: bfloat16 [4096, 8192], P('seq', 'mp'), may hold values from -6 to 6
- img_start: int32 [64], replicated, may hold values from 0 to 4092, as said below
- img_len: int32 [64], replicated, may hold values from 4 to 64, as said below
- img_owner: int32 [64], replicated, may hold values from 0 to 7, as said below
- pre_act: bfloat16 [4096, 5120], P('seq', 'mp'), may hold values from -6 to 6
- w_out: bfloat16 [5120, 8192], P(None, 'mp'), may hold values from -0.0625 to 0.0625
Outputs:
- pre_grad: bfloat16 [4096, 5120], P('seq', 'mp')
- weight_grad: bfloat16 [5120, 8192], P('seq', 'mp')
The draws below stay inside these ranges and needn't reach their ends.
Inputs may be any that keep to these rules, and one draw needn't show every extreme that they name: Image i lies inside positions i * 64 to (i + 1) * 64 - 1: img_start[i] - i * 64 + img_len[i] <= 64. `img_len`: A multiple of 4. In every draw some owner has all its images of exactly 64 merged tokens. `img_owner`: the images i with one value of i % 8 all have different owners, and so do the 8 images of one stripe (images i with one value of i // 8).
All inputs are finite; a program needn't handle non-finite values.
Results may differ from the reference program's by a relative error of at most 0.02.
Values may be sent and summed in bfloat16 or wider, within the bound.
A program may use at most 192 MiB of HBM per device.

```python
import math
import jax
import jax.numpy as jnp
from jax import lax

D_MERGE = 5120
D_OUT = 8192
STRIPE_DEV = 512
FRAME = 64
IMG_STRIPE = 8
NUM_IMG = 64
SEQ_TOT = 4096
N_SEQ = 8


def image_layout(key):
    base = jax.random.fold_in(key, 11)
    subkeys = jax.random.split(base, 4)
    stripes = NUM_IMG // IMG_STRIPE
    image_ids = jnp.arange(NUM_IMG, dtype=jnp.int32)
    lengths = 4 * jax.random.randint(subkeys[0], (NUM_IMG,), 1, FRAME // 4 + 1, dtype=jnp.int32)
    shuffle = jax.random.permutation(subkeys[1], stripes).astype(jnp.int32)
    owners = (shuffle[image_ids // IMG_STRIPE] + image_ids % IMG_STRIPE) % stripes
    chosen = jax.random.randint(subkeys[2], (), 0, stripes, dtype=jnp.int32)
    lengths = jnp.where(owners == chosen, FRAME, lengths).astype(jnp.int32)
    leftover = FRAME - lengths
    offsets = jax.random.randint(subkeys[3], (NUM_IMG,), 0, 1 << 20, dtype=jnp.int32) % (leftover + 1)
    starts = image_ids * FRAME + offsets
    return (starts.astype(jnp.int32), lengths, owners.astype(jnp.int32))


def draw_img_start(key, part):
    return image_layout(key)[0]


def draw_img_len(key, part):
    return image_layout(key)[1]


def draw_img_owner(key, part):
    return image_layout(key)[2]


def spiked(drawn, key, source, target, blocks, factor):
    def block_of(axis_at):
        return (jnp.arange(drawn.shape[axis_at]) // (drawn.shape[axis_at] // blocks)).reshape((-1,) + (1,) * (drawn.ndim - 1 - axis_at))

    one_side = jax.random.permutation(key, blocks)[block_of(target)]
    other_side = (block_of(target) + blocks // 2) % blocks
    return jnp.where((block_of(source) == one_side) | (block_of(source) == other_side), factor * drawn, drawn)


def block_scale(own_key, extent, pieces, low, top_value):
    def one(position, blocks):
        steps = jax.random.uniform(jax.random.fold_in(jax.random.fold_in(own_key, 6), position), (blocks,), jnp.float32, low / len(pieces), top_value / len(pieces))
        return jnp.repeat(jnp.exp(steps), extent[position] // blocks).reshape((-1,) + (1,) * (len(extent) - position - 1))

    level = one(*pieces[0])
    for cut in pieces[1:]:
        level = level * one(*cut)
    return level


def bell_draw(own_key, dims, deviation, limit, shards=(), kind=jnp.bfloat16):
    array = deviation * jax.random.normal(own_key, dims, jnp.float32)
    if shards:
        array = array * block_scale(own_key, dims, shards, -0.22, 0.18)
    return jnp.clip(array, -limit, limit).astype(kind)


def noise_with(key, extent, deviation, most, shards, heavy, kind=jnp.bfloat16):
    drawn = deviation * jax.random.normal(key, extent, jnp.float32)
    if shards:
        drawn = drawn * block_scale(key, extent, shards, -0.22, 0.18)
    return jnp.clip(spiked(drawn, jax.random.fold_in(key, 3), *heavy), -most, most).astype(kind)


def setup_inputs(seed: int = 0) -> dict:
    seeds = jax.random.split(jax.random.key(seed), 7)
    grad_rows = bell_draw(seeds[0], (SEQ_TOT, D_OUT), 1.0, 6.0, ((0, 8), (1, 4)))
    img_start = draw_img_start(jax.random.fold_in(seeds[6], 71), 0)
    img_len = draw_img_len(jax.random.fold_in(seeds[6], 71), 0)
    img_owner = draw_img_owner(jax.random.fold_in(seeds[6], 71), 0)
    pre_act = noise_with(seeds[4], (SEQ_TOT, D_MERGE), 1.0, 6.0, ((0, 8), (1, 4)), (0, 1, 8, 2.0))
    w_out = bell_draw(seeds[5], (D_MERGE, D_OUT), D_OUT ** -0.5, 0.0625, ((1, 4),))
    return dict(grad_rows=grad_rows, img_start=img_start, img_len=img_len, img_owner=img_owner, pre_act=pre_act, w_out=w_out)


def gelu_parts(values):
    normal_cdf = 0.5 * (1.0 + lax.erf(values * 0.7071067811865476))
    density = jnp.exp(-0.5 * values * values) * 0.3989422804014327
    return (values * normal_cdf, normal_cdf + values * density)

def reference(grad_rows, img_start, img_len, img_owner, pre_act, w_out):
    frames = STRIPE_DEV // FRAME
    image_ids = jnp.arange(NUM_IMG, dtype=jnp.int32)
    within = jnp.arange(FRAME, dtype=jnp.int32)
    slot_ids = (img_owner * STRIPE_DEV + image_ids % frames * FRAME)[:, None] + within[None, :]
    positions = jnp.clip(img_start[:, None] + within[None, :], 0, SEQ_TOT - 1).astype(jnp.int32)
    filled = within[None, :] < img_len[:, None]
    picked = jnp.where(filled[:, :, None], grad_rows[positions], jnp.zeros((), jnp.bfloat16))
    routed = jnp.zeros((SEQ_TOT, D_OUT), jnp.bfloat16).at[slot_ids.reshape(-1)].set(picked.reshape(-1, D_OUT))
    hidden_grad = lax.dot_general(routed, w_out, (((1,), (1,)), ((), ())), preferred_element_type=jnp.float32)
    activation, derivative = gelu_parts(pre_act.astype(jnp.float32))
    activation = activation.astype(jnp.bfloat16)
    pre_grad = (hidden_grad * derivative).astype(jnp.bfloat16)
    factor = 1.0 / math.sqrt(SEQ_TOT)

    def accumulate(running, owner_block):
        owner_act, owner_rows = owner_block
        partial_value = lax.dot_general(owner_act, owner_rows, (((0,), (0,)), ((), ())), preferred_element_type=jnp.float32) * factor
        partial_value = lax.optimization_barrier(partial_value.astype(jnp.bfloat16))
        return (running + partial_value.astype(jnp.float32), None)
    weight_grad, _ = lax.scan(accumulate, jnp.zeros((D_MERGE, D_OUT), jnp.float32), (activation.reshape(N_SEQ, STRIPE_DEV, D_MERGE), routed.reshape(N_SEQ, STRIPE_DEV, D_OUT)))
    return (pre_grad, weight_grad.astype(jnp.bfloat16))
```

```python
import functools
import math

import jax
import jax.numpy as jnp
from jax import lax
from jax.experimental import pallas as pl
from jax.experimental.pallas import tpu as pltpu
from jax.sharding import PartitionSpec as P

FRAME = 64
MESH = pl.DeviceIdType.MESH


def gelu_parts(values):
    normal_cdf = 0.5 * (1.0 + lax.erf(values * 0.7071067811865476))
    density = jnp.exp(-0.5 * values * values) * 0.3989422804014327
    return (values * normal_cdf, normal_cdf + values * density)


def exchange_kernel(
    n, mp, inner, pieces,
    rows_ref, act_ref, place_ref, w_ref,
    rows_out, act_out, hid_out,
    terms_ref, parts, outbuf, w_buf, w_sem,
    rs_recv, rs_send, row_recv, row_send, act_recv, act_send, act_fwd, act_own,
    hid_recv, hid_send, local_sem,
):
    s = lax.axis_index("seq")
    m = lax.axis_index("mp")
    outer = n // inner
    z, xi = s // inner, s % inner
    stripe = rows_ref.shape[0]
    piece = stripe // pieces
    tokens = act_ref.shape[1]
    half = tokens // 2
    per = act_ref.shape[0]
    xfirst = inner == 2
    seq_peers = [((s + q) % n, m) for q in range(1, n)]
    mp_peers = [(s, (m + q) % mp) for q in range(1, mp)]

    opposite = (m + mp // 2) % mp
    greeted = seq_peers + mp_peers + [((s + q) % n, opposite) for q in range(1, n)]
    barrier = pltpu.get_barrier_semaphore()
    for peer in greeted:
        pl.semaphore_signal(barrier, inc=1, device_id=peer, device_id_type=MESH)
    pl.semaphore_wait(barrier, len(greeted))

    def remote(src, dst, send, recv, peer):
        return pltpu.make_async_remote_copy(
            src_ref=src, dst_ref=dst, send_sem=send, recv_sem=recv,
            device_id=peer, device_id_type=MESH,
        )

    def row_copy(t, p, way, peer, own=False):
        slot = rows_out.at[pl.ds(t * stripe + p * piece, piece)]
        src = rows_ref.at[pl.ds(p * piece, piece)] if own else slot
        return remote(src, slot, row_send.at[t, p, way], row_recv.at[t, p], peer)

    def go(run, copy):
        if run:
            copy.start()
        else:
            copy.wait_send()

    def arrive(run, t, p):
        if run:
            row_copy(t, p, 0, ((s + 1) % n, m)).wait_recv()

    def up(run, t, p, own=False):
        @pl.when(z < outer - 1)
        def _():
            go(run, row_copy(t, p, 0, (s + inner, m), own))

    def down(run, t, p, own=False):
        @pl.when(z > 0)
        def _():
            go(run, row_copy(t, p, 1, (s - inner, m), own))

    def across(run, t, p, own=False):
        for q in range(1, inner):
            go(run, row_copy(t, p, 1 + q, (z * inner + (xi + q) % inner, m), own))

    def loop(first, body):
        def step(p, carry):
            body(p)
            return carry
        lax.fori_loop(first, pieces, step, 0)

    def own_rows(run):
        def body(p):
            up(run, s, p, True)
            down(run, s, p, True)
            across(run, s, p, True)
        loop(0, body)

    def partner_rows(run):
        if xfirst:
            t = z * inner + (1 - xi)
            for p in range(2):
                arrive(run, t, p)
                up(run, t, p)
                down(run, t, p)

    def hop(run, d):
        def one(p, crossing):
            @pl.when(z >= d)
            def _():
                t = s - d * inner
                arrive(run, t, p)
                up(run, t, p)
                if crossing:
                    across(run, t, p)
                else:
                    t2 = (z - d) * inner + (1 - xi)
                    arrive(run, t2, p)
                    up(run, t2, p)

            @pl.when(z + d < outer)
            def _():
                t = s + d * inner
                arrive(run, t, p)
                down(run, t, p)
                if crossing:
                    across(run, t, p)
                else:
                    t2 = (z + d) * inner + (1 - xi)
                    arrive(run, t2, p)
                    down(run, t2, p)

        if xfirst:
            one(0, False)
            one(1, False)
            loop(2, lambda p: one(p, True))
        else:
            loop(0, lambda p: one(p, True))

    def rest_rows():
        for zz in range(outer):
            for q in range(1, inner):
                t = zz * inner + (xi + q) % inner
                loop(2 if xfirst else 0, lambda p: arrive(True, t, p))

    root_a = s // per
    root_b = (root_a + mp // 2) % mp

    def act_slot(t, h):
        return act_out.at[pl.ds(t * tokens + h * half, half)]

    def act_first(run):
        for j in range(per):
            target = m * per + j

            @pl.when(target != s)
            def _():
                for h, to in ((0, m), (1, opposite)):
                    go(run, remote(
                        act_ref.at[j, pl.ds(h * half, half)], act_slot(s, h),
                        act_send.at[j, h], act_recv.at[s, h], (target, to),
                    ))

            @pl.when(target == s)
            def _():
                for h in range(2):
                    for q, peer in enumerate(mp_peers):
                        go(run, remote(
                            act_ref.at[j, pl.ds(h * half, half)], act_slot(s, h),
                            act_own.at[h, q], act_recv.at[s, h], peer,
                        ))
                mine = pltpu.make_async_copy(
                    act_ref.at[j], act_out.at[pl.ds(s * tokens, tokens)], local_sem.at[1]
                )
                if run:
                    mine.start()
                else:
                    mine.wait()

    def act_wait(t, h):
        remote(act_slot(t, h), act_slot(t, h), act_fwd.at[0, 0], act_recv.at[t, h], mp_peers[0]).wait_recv()

    def act_pass(run):
        for h, root in ((0, root_a), (1, root_b)):
            @pl.when(m == root)
            def _():
                for k in range(1, n):
                    t = (s + k) % n
                    if run:
                        act_wait(t, h)
                    for q, peer in enumerate(mp_peers):
                        go(run, remote(
                            act_slot(t, h), act_slot(t, h), act_fwd.at[t, q], act_recv.at[t, h], peer,
                        ))

    def act_rest():
        for h, root in ((0, root_a), (1, root_b)):
            @pl.when(m != root)
            def _():
                for k in range(1, n):
                    act_wait((s + k) % n, h)

            @pl.when(m != root_a)
            def _():
                act_wait(s, h)

    def sums(run):
        for q, peer in enumerate(mp_peers):
            go(run, remote(terms_ref.at[peer[1]], parts.at[m], rs_send.at[q], rs_recv.at[m], peer))

    def hid_copy(q):
        peer = ((s + q) % n, m)
        return remote(
            outbuf.at[pl.ds(pl.multiple_of(peer[0] * FRAME, FRAME), FRAME)],
            hid_out.at[pl.ds(pl.multiple_of(s * FRAME, FRAME), FRAME)],
            hid_send.at[q], hid_recv.at[s], peer,
        )

    def hid_mine():
        at = pl.ds(pl.multiple_of(s * FRAME, FRAME), FRAME)
        return pltpu.make_async_copy(outbuf.at[at], hid_out.at[at], local_sem.at[2])

    def hidden():
        for q, peer in enumerate(mp_peers):
            remote(terms_ref.at[0], parts.at[peer[1]], rs_send.at[q], rs_recv.at[peer[1]], peer).wait_recv()
        width = parts.shape[2]
        chunk = 256 if width % 256 == 0 else width

        def step(c, carry):
            at = pl.ds(pl.multiple_of(c * chunk, chunk), chunk)
            total = terms_ref[m, :, at].astype(jnp.float32)
            for q in range(1, mp):
                total = total + parts[(m + q) % mp, :, at].astype(jnp.float32)
            outbuf[:, at] = jnp.dot(
                place_ref[...], total.astype(jnp.bfloat16), preferred_element_type=jnp.float32
            ).astype(jnp.bfloat16)
            return carry

        lax.fori_loop(0, width // chunk, step, 0)

    def hid_wait(t):
        at = pl.ds(pl.multiple_of(t * FRAME, FRAME), FRAME)
        remote(outbuf.at[pl.ds(0, FRAME)], hid_out.at[at], hid_send.at[1], hid_recv.at[t], seq_peers[0]).wait_recv()

    def multiply():
        width = terms_ref.shape[2]
        tile = w_buf.shape[1]
        per_part = width // tile

        def where(c):
            return (m + 1 + c // per_part) % mp, (c % per_part) * tile

        def fetch(c, slot):
            q, col = where(c)
            at = pl.ds(pl.multiple_of(q * width + col, tile), tile)
            return pltpu.make_async_copy(w_ref.at[at], w_buf.at[slot], w_sem.at[slot])

        count = mp * per_part
        fetch(0, 0).start()

        def step(c, carry):
            slot = c % 2

            @pl.when(c + 1 < count)
            def _():
                fetch(c + 1, 1 - slot).start()
            fetch(c, slot).wait()
            q, col = where(c)
            terms_ref[q, :, pl.ds(pl.multiple_of(col, tile), tile)] = lax.dot_general(
                rows_ref[...], w_buf[slot], (((1,), (1,)), ((), ())),
                preferred_element_type=jnp.float32,
            ).astype(jnp.bfloat16)
            return carry

        lax.fori_loop(0, count, step, 0)

    keep = pltpu.make_async_copy(rows_ref, rows_out.at[pl.ds(s * stripe, stripe)], local_sem.at[0])
    act_first(True)
    own_rows(True)
    keep.start()
    partner_rows(True)
    multiply()
    sums(True)
    hop(True, 1)
    act_pass(True)
    hidden()
    hop(True, 2)
    for q in range(1, n):
        hid_copy(q).start()
    hid_mine().start()
    for d in range(3, outer):
        hop(True, d)
    rest_rows()
    act_rest()
    for q in range(1, n):
        hid_wait((s + q) % n)

    keep.wait()
    hid_mine().wait()
    own_rows(False)
    sums(False)
    act_first(False)
    partner_rows(False)
    for d in range(1, outer):
        hop(False, d)
    act_pass(False)
    for q in range(1, n):
        hid_copy(q).wait_send()


def exchange(n, mp, tag, rows, acts, place, w_out):
    stripe, quarter = rows.shape
    per, tokens, kept = acts.shape
    width = w_out.shape[0] // mp
    inner = n // 4
    pieces = stripe // 32 if inner == 2 else 1
    vm = pl.BlockSpec(memory_space=pltpu.VMEM)
    anywhere = pl.BlockSpec(memory_space=pl.ANY)
    dma = pltpu.SemaphoreType.DMA
    return pl.pallas_call(
        functools.partial(exchange_kernel, n, mp, inner, pieces),
        out_shape=(
            jax.ShapeDtypeStruct((n * stripe, quarter), jnp.bfloat16),
            jax.ShapeDtypeStruct((n * tokens, kept), jnp.bfloat16),
            jax.ShapeDtypeStruct((n * FRAME, width), jnp.bfloat16),
        ),
        in_specs=[vm] * 3 + [anywhere],
        out_specs=(anywhere,) * 3,
        scratch_shapes=[
            pltpu.VMEM((mp, stripe, width), jnp.bfloat16),
            pltpu.VMEM((mp, stripe, width), jnp.bfloat16),
            pltpu.VMEM((n * FRAME, width), jnp.bfloat16),
            pltpu.VMEM((2, 256 if width % 256 == 0 else width, quarter), jnp.bfloat16),
            dma((2,)),
            dma((mp,)), dma((mp,)),
            dma((n, pieces)), dma((n, pieces, 1 + inner)),
            dma((n, 2)), dma((per, 2)), dma((n, mp)), dma((2, mp)),
            dma((n,)), dma((n,)), dma((3,)),
        ],
        compiler_params=pltpu.CompilerParams(
            collective_id=tag, has_side_effects=True, vmem_limit_bytes=60 * 1024 * 1024
        ),
    )(rows, acts, place, w_out)


def spread(counts, before, base, size):
    r = jnp.arange(size, dtype=jnp.int32)
    inside = (r >= before[..., None]) & (r < (before + counts)[..., None])
    return jnp.sum(jnp.where(inside, (base - before)[..., None] + r + 1, 0), axis=-2) - 1


def local(n, mp, grad_rows, img_start, img_len, img_owner, pre_act, w_out):
    stripe, quarter = grad_rows.shape
    width = pre_act.shape[1]
    kept = w_out.shape[0] // n
    frames = stripe // FRAME
    here = lax.axis_index("seq")
    owner = img_owner.reshape(n, frames)
    starts = img_start.reshape(n, frames)
    lengths = img_len.reshape(n, frames)
    before = jnp.cumsum(lengths, axis=1) - lengths
    row = jnp.arange(FRAME, dtype=jnp.int32)
    column = jnp.arange(stripe, dtype=jnp.int32)

    values = pre_act.astype(jnp.float32)
    activation, derivative = gelu_parts(values)
    activation = activation.astype(jnp.bfloat16)
    acts = activation.reshape(stripe, width // kept, kept).transpose(1, 0, 2)

    my_owner = lax.dynamic_slice_in_dim(owner, here, 1)[0]
    my_start = lax.dynamic_slice_in_dim(starts, here, 1)[0] - here * stripe
    my_length = lax.dynamic_slice_in_dim(lengths, here, 1)[0]
    my_before = lax.dynamic_slice_in_dim(before, here, 1)[0]
    to = (my_owner[None, :] == jnp.arange(n, dtype=jnp.int32)[:, None]).astype(jnp.int32)
    first = jnp.sum(to * my_before[None, :], axis=1)
    count = jnp.sum(to * my_length[None, :], axis=1)
    at = jnp.where(row[None, :] < count[:, None], first[:, None] + row[None, :], -1).reshape(n * FRAME, 1)
    order = img_owner * frames + jnp.arange(n * frames, dtype=jnp.int32) % frames
    factor = 1.0 / math.sqrt(n * stripe)

    def with_size(tag, size, grad_rows, acts, w_out):
        source = spread(my_length, my_before, my_start, size)
        live = (source[:, None] == column[None, :]).astype(jnp.bfloat16)
        rows = jnp.dot(live, grad_rows, preferred_element_type=jnp.float32).astype(jnp.bfloat16)
        place = (at == jnp.arange(size, dtype=jnp.int32)[None, :]).astype(jnp.bfloat16)
        rows_all, act_all, hid = exchange(n, mp, tag, rows, acts, place, w_out)
        blocks = act_all.reshape(n * frames, FRAME, kept)[order].reshape(n, stripe, kept)
        block = jnp.broadcast_to(jnp.arange(frames, dtype=jnp.int32) * FRAME, (n, frames))
        taken = spread(lengths, before, block, size)
        lined = (taken[:, :, None] == column[None, None, :]).astype(jnp.bfloat16)
        act_rows = jnp.einsum(
            "trc,tck->trk", lined, blocks, preferred_element_type=jnp.float32
        ).astype(jnp.bfloat16).reshape(n * size, kept)
        product = lax.dot_general(
            act_rows, rows_all, (((0,), (0,)), ((), ())), preferred_element_type=jnp.float32
        ) * factor
        return lax.optimization_barrier(product.astype(jnp.bfloat16)), hid

    sizes = [stripe // 16 * k for k in (12, 13, 16)]
    most = jnp.max(jnp.sum(lengths, axis=1))
    which = sum((most > size).astype(jnp.int32) for size in sizes[:-1])
    weight_grad, hid = lax.switch(
        which,
        [functools.partial(with_size, tag, size) for tag, size in enumerate(sizes)],
        grad_rows, acts, w_out,
    )

    came = jnp.arange(n * FRAME, dtype=jnp.int32)
    from_me = (owner == here).T
    pick = jnp.repeat(jnp.repeat(from_me, FRAME, axis=0), FRAME, axis=1)
    pick = (pick & (column[:, None] % FRAME == came[None, :] % FRAME)).astype(jnp.bfloat16)
    hidden_grad = jnp.dot(pick, hid, preferred_element_type=jnp.float32)
    pre_grad = (hidden_grad * derivative).astype(jnp.bfloat16)
    return (pre_grad, weight_grad)


def fused_kernel(
    n, mp, inner, pieces, early, factor,
    order_ref, rows_ref, act_ref, place_ref, taken_ref, w_ref,
    hid_out, grad_out,
    rows_all, act_all, w_all, acc, hot, block, lined, picked, terms, parts, hid, stage,
    w_sem, rs_recv, rs_send, row_recv, row_send, act_recv, act_send, act_fwd, act_own,
    local_sem, out_sem,
):
    s = lax.axis_index("seq")
    m = lax.axis_index("mp")
    outer = n // inner
    z, xi = s // inner, s % inner
    size = rows_ref.shape[0]
    piece = size // pieces
    per, frames, _, kept = act_ref.shape
    half = frames // 2
    quarter = rows_ref.shape[1]
    width = parts.shape[3]
    seq_peers = [((s + q) % n, m) for q in range(1, n)]
    mp_peers = [(s, (m + q) % mp) for q in range(1, mp)]
    opposite = (m + mp // 2) % mp
    greeted = seq_peers + mp_peers + [((s + q) % n, opposite) for q in range(1, n)]
    barrier = pltpu.get_barrier_semaphore()
    for peer in greeted:
        pl.semaphore_signal(barrier, inc=1, device_id=peer, device_id_type=MESH)
    pl.semaphore_wait(barrier, len(greeted))

    def remote(src, dst, send, recv, peer):
        return pltpu.make_async_remote_copy(
            src_ref=src, dst_ref=dst, send_sem=send, recv_sem=recv,
            device_id=peer, device_id_type=MESH,
        )

    def row_copy(t, p, way, peer, own=False):
        slot = rows_all.at[t, pl.ds(p * piece, piece)]
        src = rows_ref.at[pl.ds(p * piece, piece)] if own else slot
        return remote(src, slot, row_send.at[t, p, way], row_recv.at[t, p], peer)

    def go(run, copy):
        if run:
            copy.start()
        else:
            copy.wait_send()

    def arrive(run, t, p):
        if run:
            row_copy(t, p, 0, ((s + 1) % n, m)).wait_recv()

    def up(run, t, p, own=False):
        @pl.when(z < outer - 1)
        def _():
            go(run, row_copy(t, p, 0, (s + inner, m), own))

    def down(run, t, p, own=False):
        @pl.when(z > 0)
        def _():
            go(run, row_copy(t, p, 1, (s - inner, m), own))

    def across(run, t, p, own=False):
        go(run, row_copy(t, p, 2, (z * inner + 1 - xi, m), own))

    def loop(first, last, body):
        def step(p, carry):
            body(p)
            return carry
        lax.fori_loop(first, last, step, 0)

    def own_rows(run):
        def body(p):
            up(run, s, p, True)
            down(run, s, p, True)
            across(run, s, p, True)
        loop(0, pieces, body)

    def partner_rows(run):
        t = z * inner + (1 - xi)
        for p in range(early):
            arrive(run, t, p)
            up(run, t, p)
            down(run, t, p)

    def hop(run, d, first, last):
        def one(p, crossing):
            @pl.when(z >= d)
            def _():
                t = s - d * inner
                arrive(run, t, p)
                up(run, t, p)
                if crossing:
                    across(run, t, p)
                else:
                    t2 = (z - d) * inner + (1 - xi)
                    arrive(run, t2, p)
                    up(run, t2, p)

            @pl.when(z + d < outer)
            def _():
                t = s + d * inner
                arrive(run, t, p)
                down(run, t, p)
                if crossing:
                    across(run, t, p)
                else:
                    t2 = (z + d) * inner + (1 - xi)
                    arrive(run, t2, p)
                    down(run, t2, p)

        for p in range(first, min(last, early)):
            one(p, False)
        loop(max(first, early), last, lambda p: one(p, True))

    def rest(layer):
        t = layer * inner + (1 - xi)
        loop(early, pieces, lambda p: arrive(True, t, p))

    root_a = s // per
    root_b = (root_a + mp // 2) % mp

    def act_slot(t, h):
        return act_all.at[pl.ds(t * frames + h * half, half)]

    def act_piece(j, h):
        return act_ref.at[j, pl.ds(h * half, half)]

    def act_mine(j):
        return pltpu.make_async_copy(
            act_ref.at[j], act_all.at[pl.ds(s * frames, frames)], local_sem.at[1]
        )

    def act_first(run):
        for j in range(per):
            target = m * per + j

            @pl.when(target != s)
            def _():
                for h, to in ((0, m), (1, opposite)):
                    go(run, remote(
                        act_piece(j, h), act_slot(s, h),
                        act_send.at[j, h], act_recv.at[s, h], (target, to),
                    ))

            @pl.when(target == s)
            def _():
                for h in range(2):
                    for q, peer in enumerate(mp_peers):
                        go(run, remote(
                            act_piece(j, h), act_slot(s, h),
                            act_own.at[h, q], act_recv.at[s, h], peer,
                        ))
                if run:
                    act_mine(j).start()

    def act_wait(t, h):
        remote(act_slot(t, h), act_slot(t, h), act_fwd.at[0, 0], act_recv.at[t, h], mp_peers[0]).wait_recv()

    def act_pass(run):
        for h, root in ((0, root_a), (1, root_b)):
            @pl.when(m == root)
            def _():
                for k in range(1, n):
                    t = (s + k) % n
                    if run:
                        act_wait(t, h)
                    for q, peer in enumerate(mp_peers):
                        go(run, remote(
                            act_slot(t, h), act_slot(t, h), act_fwd.at[t, q], act_recv.at[t, h], peer,
                        ))

    def act_rest():
        for h, root in ((0, root_a), (1, root_b)):
            @pl.when(m != root)
            def _():
                for k in range(1, n):
                    act_wait((s + k) % n, h)

            @pl.when(m != root_a)
            def _():
                act_wait(s, h)

        @pl.when(m == root_a)
        def _():
            act_mine(s % per).wait()

    def layer_of(k):
        if k == 0:
            return z
        low = outer // 2
        if k == 1:
            return jnp.where(z < low, low - 1 - z, 3 * low - 1 - z)
        return jnp.where(z < low, k, outer - 1 - k)

    def sums(run, g):
        for q, peer in enumerate(mp_peers):
            part_copy(run, g, q, peer)

    def part_copy(run, g, q, peer):
        go(run, remote(
            terms.at[peer[1]], parts.at[g, m], rs_send.at[g, q], rs_recv.at[g, m], peer,
        ))

    def select(layer):
        tile = 512 if quarter % 512 == 0 else quarter
        for j in range(inner):
            t = layer * inner + j

            def step(c):
                at = pl.ds(pl.multiple_of(c * tile, tile), tile)
                picked[pl.ds(j * FRAME, FRAME), at] = jnp.dot(
                    place_ref[pl.ds(pl.multiple_of(t * FRAME, FRAME), FRAME), :],
                    rows_all[t, :, at], preferred_element_type=jnp.float32,
                ).astype(jnp.bfloat16)
            loop(0, quarter // tile, step)

    def hidden(g, layer):
        select(layer)
        if g > 0:
            sums(False, g - 1)
        tile = 256 if width % 256 == 0 else width
        for q in range(mp):
            to = (m + 1 + q) % mp

            def step(c):
                col = pl.multiple_of(c * tile, tile)
                value = lax.dot_general(
                    picked[...], w_all[pl.ds(pl.multiple_of(to * width + c * tile, tile), tile), :],
                    (((1,), (1,)), ((), ())), preferred_element_type=jnp.float32,
                ).astype(jnp.bfloat16)
                if q < mp - 1:
                    terms[to, :, pl.ds(col, tile)] = value
                else:
                    parts[g, m, :, pl.ds(col, tile)] = value
            loop(0, width // tile, step)
            if q > 0:
                part_copy(True, g, q - 1, mp_peers[q - 1])

    def reduce(g, layer):
        for q, peer in enumerate(mp_peers):
            remote(
                terms.at[0], parts.at[g, peer[1]], rs_send.at[g, q], rs_recv.at[g, peer[1]], peer
            ).wait_recv()
        tile = 256 if width % 256 == 0 else width
        for j in range(inner):
            t = layer * inner + j

            def step(c):
                at = pl.ds(pl.multiple_of(c * tile, tile), tile)
                rows = pl.ds(j * FRAME, FRAME)
                total = parts[g, 0, rows, at].astype(jnp.float32)
                for q in range(1, mp):
                    total = total + parts[g, q, rows, at].astype(jnp.float32)
                hid[t, :, at] = total.astype(jnp.bfloat16)
            loop(0, width // tile, step)

    def line_up(layer):
        for j in range(inner):
            t = layer * inner + j

            def frame(f):
                at = pl.ds(pl.multiple_of(f * FRAME, FRAME), FRAME)
                block[at, :] = act_all[order_ref[t * frames + f]]
                row = lax.broadcasted_iota(jnp.int32, (FRAME, size), 0) + f * FRAME
                hot[at, :] = jnp.where(row == taken_ref[t], 1.0, 0.0).astype(jnp.bfloat16)
            loop(0, frames, frame)

            def step(c):
                at = pl.ds(pl.multiple_of(c * 128, 128), 128)
                lined[j, at, :] = lax.dot_general(
                    block[:, at], hot[...], (((0,), (0,)), ((), ())),
                    preferred_element_type=jnp.float32,
                ).astype(jnp.bfloat16)
            loop(0, kept // 128, step)

    def weights(g, layer, last):
        line_up(layer)
        tile = 256 if quarter % 256 == 0 else quarter
        count = quarter // tile

        def put(c, slot):
            at = pl.ds(pl.multiple_of(c * tile, tile), tile)
            return pltpu.make_async_copy(stage.at[slot], grad_out.at[:, at], out_sem.at[slot])

        def step(c):
            at = pl.ds(pl.multiple_of(c * tile, tile), tile)
            value = jnp.dot(lined[0], rows_all[layer * inner, :, at], preferred_element_type=jnp.float32)
            for j in range(1, inner):
                value = value + jnp.dot(
                    lined[j], rows_all[layer * inner + j, :, at], preferred_element_type=jnp.float32
                )
            if g > 0:
                value = value + acc[:, at]
            if not last:
                acc[:, at] = value
                return
            slot = c % 2

            @pl.when(c > 1)
            def _():
                put(c - 2, slot).wait()
            stage[slot] = (value * factor).astype(jnp.bfloat16)
            put(c, slot).start()
        loop(0, count, step)
        if last:
            for c in range(max(0, count - 2), count):
                put(c, c % 2).wait()

    fetch = pltpu.make_async_copy(w_ref, w_all, w_sem)
    keep = pltpu.make_async_copy(rows_ref, rows_all.at[s], local_sem.at[0])
    act_first(True)
    own_rows(True)
    keep.start()
    fetch.start()
    partner_rows(True)
    act_pass(True)
    hop(True, 1, 0, pieces)
    keep.wait()
    fetch.wait()
    rest(layer_of(0))
    hidden(0, layer_of(0))
    rest(layer_of(1))
    act_rest()
    weights(0, layer_of(0), False)
    reduce(0, layer_of(0))
    hidden(1, layer_of(1))
    weights(1, layer_of(1), False)
    hop(True, 2, 0, pieces)
    rest(layer_of(2))
    reduce(1, layer_of(1))
    hidden(2, layer_of(2))
    weights(2, layer_of(2), False)
    hop(True, 3, 0, pieces)
    rest(layer_of(3))
    reduce(2, layer_of(2))
    hidden(3, layer_of(3))
    weights(3, layer_of(3), True)
    reduce(3, layer_of(3))
    for f in range(frames):
        hid_out[pl.ds(f * FRAME, FRAME), :] = hid[order_ref[n * frames + f]]

    act_first(False)
    own_rows(False)
    sums(False, outer - 1)
    partner_rows(False)
    for d in range(1, outer):
        hop(False, d, 0, pieces)
    act_pass(False)


def fused(n, mp, tag, factor, order, rows, acts, place, taken, w_out):
    stripe, quarter = rows.shape
    per, frames, _, kept = acts.shape
    width = w_out.shape[0] // mp
    inner = n // 4
    outer = n // inner
    pieces = stripe // 32
    vm = pl.BlockSpec(memory_space=pltpu.VMEM)
    anywhere = pl.BlockSpec(memory_space=pl.ANY)
    dma = pltpu.SemaphoreType.DMA
    b16 = jnp.bfloat16
    return pl.pallas_call(
        functools.partial(fused_kernel, n, mp, inner, pieces, 1, factor),
        out_shape=(
            jax.ShapeDtypeStruct((frames * FRAME, width), b16),
            jax.ShapeDtypeStruct((kept, quarter), b16),
        ),
        in_specs=[pl.BlockSpec(memory_space=pltpu.SMEM)] + [vm] * 4 + [anywhere],
        out_specs=(vm, anywhere),
        scratch_shapes=[
            pltpu.VMEM((n, stripe, quarter), b16),
            pltpu.VMEM((n * frames, FRAME, kept), b16),
            pltpu.VMEM(w_out.shape, b16),
            pltpu.VMEM((kept, quarter), jnp.float32),
            pltpu.VMEM((frames * FRAME, stripe), b16),
            pltpu.VMEM((frames * FRAME, kept), b16),
            pltpu.VMEM((inner, kept, stripe), b16),
            pltpu.VMEM((inner * FRAME, quarter), b16),
            pltpu.VMEM((mp, inner * FRAME, width), b16),
            pltpu.VMEM((outer, mp, inner * FRAME, width), b16),
            pltpu.VMEM((n, FRAME, width), b16),
            pltpu.VMEM((2, kept, 256 if quarter % 256 == 0 else quarter), b16),
            dma(()), dma((outer, mp)), dma((outer, mp)),
            dma((n, pieces)), dma((n, pieces, 3)),
            dma((n, 2)), dma((per, 2)), dma((n, mp)), dma((2, mp)),
            dma((2,)), dma((2,)),
        ],
        compiler_params=pltpu.CompilerParams(
            collective_id=tag, has_side_effects=True, vmem_limit_bytes=67043328
        ),
    )(order, rows, acts, place, taken, w_out)


def local_fused(n, mp, grad_rows, img_start, img_len, img_owner, pre_act, w_out):
    stripe, quarter = grad_rows.shape
    width = pre_act.shape[1]
    kept = w_out.shape[0] // n
    frames = stripe // FRAME
    per = width // kept
    here = lax.axis_index("seq")
    owner = img_owner.reshape(n, frames)
    starts = img_start.reshape(n, frames)
    lengths = img_len.reshape(n, frames)
    before = jnp.cumsum(lengths, axis=1) - lengths
    row = jnp.arange(FRAME, dtype=jnp.int32)
    column = jnp.arange(stripe, dtype=jnp.int32)

    values = pre_act.astype(jnp.float32)
    activation, derivative = gelu_parts(values)
    activation = activation.astype(jnp.bfloat16)
    acts = activation.reshape(stripe, per, kept).transpose(1, 0, 2).reshape(per, frames, FRAME, kept)

    my_start = lax.dynamic_slice_in_dim(starts, here, 1)[0] - here * stripe
    my_length = lax.dynamic_slice_in_dim(lengths, here, 1)[0]
    my_before = lax.dynamic_slice_in_dim(before, here, 1)[0]
    mine = (owner == here).astype(jnp.int32)
    first = jnp.sum(mine * before, axis=1)
    count = jnp.sum(mine * lengths, axis=1)
    at = jnp.where(row[None, :] < count[:, None], first[:, None] + row[None, :], -1).reshape(n * FRAME, 1)
    source_of = jnp.sum(mine * jnp.arange(n, dtype=jnp.int32)[:, None], axis=0)
    order = img_owner * frames + jnp.arange(n * frames, dtype=jnp.int32) % frames
    order = jnp.concatenate([order, source_of])
    factor = 1.0 / math.sqrt(n * stripe)
    block = jnp.broadcast_to(jnp.arange(frames, dtype=jnp.int32) * FRAME, (n, frames))

    def with_size(tag, size, grad_rows, acts, w_out):
        source = spread(my_length, my_before, my_start, size)
        live = (source[:, None] == column[None, :]).astype(jnp.bfloat16)
        rows = jnp.dot(live, grad_rows, preferred_element_type=jnp.float32).astype(jnp.bfloat16)
        place = (at == jnp.arange(size, dtype=jnp.int32)[None, :]).astype(jnp.bfloat16)
        taken = spread(lengths, before, block, size).reshape(n, 1, size)
        return fused(n, mp, tag, factor, order, rows, acts, place, taken, w_out)

    sizes = [stripe // 16 * k for k in (12, 13, 16)]
    most = jnp.max(jnp.sum(lengths, axis=1))
    which = sum((most > size).astype(jnp.int32) for size in sizes[:-1])
    hid, weight_grad = lax.switch(
        which,
        [functools.partial(with_size, tag, size) for tag, size in enumerate(sizes)],
        grad_rows, acts, w_out,
    )
    pre_grad = (hid.astype(jnp.float32) * derivative).astype(jnp.bfloat16)
    return (pre_grad, weight_grad)


def chosen(n, mp, grad_rows, *rest):
    whole = n * grad_rows.shape[0] * grad_rows.shape[1] + rest[-1].shape[0] * rest[-1].shape[1]
    fits = n * FRAME == grad_rows.shape[0] and 2 * whole <= 40 * 1024 * 1024
    return (local_fused if fits else local)(n, mp, grad_rows, *rest)


def solution(mesh):
    return jax.shard_map(
        functools.partial(chosen, mesh.shape["seq"], mesh.shape["mp"]),
        mesh=mesh,
        in_specs=(P("seq", "mp"), P(), P(), P(), P("seq", "mp"), P(None, "mp")),
        out_specs=(P("seq", "mp"), P("seq", "mp")),
        check_vma=False,
    )
```

```python
import functools
import math

import jax
import jax.numpy as jnp
from jax import lax
from jax.experimental import pallas as pl
from jax.experimental.pallas import tpu as pltpu
from jax.sharding import PartitionSpec as P

FRAME = 64
MESH = pl.DeviceIdType.MESH


def gelu_parts(values):
    normal_cdf = 0.5 * (1.0 + lax.erf(values * 0.7071067811865476))
    density = jnp.exp(-0.5 * values * values) * 0.3989422804014327
    return (values * normal_cdf, normal_cdf + values * density)


def exchange_kernel(
    n, mp, inner, pieces,
    rows_ref, act_ref, place_ref, w_ref,
    rows_out, act_out, hid_out,
    terms_ref, parts, outbuf, w_buf, w_sem,
    rs_recv, rs_send, row_recv, row_send, act_recv, act_send, act_fwd, act_own,
    hid_recv, hid_send, local_sem,
):
    s = lax.axis_index("seq")
    m = lax.axis_index("mp")
    outer = n // inner
    z, xi = s // inner, s % inner
    stripe = rows_ref.shape[0]
    piece = stripe // pieces
    tokens = act_ref.shape[1]
    half = tokens // 2
    per = act_ref.shape[0]
    xfirst = inner == 2
    seq_peers = [((s + q) % n, m) for q in range(1, n)]
    mp_peers = [(s, (m + q) % mp) for q in range(1, mp)]

    opposite = (m + mp // 2) % mp
    greeted = seq_peers + mp_peers + [((s + q) % n, opposite) for q in range(1, n)]
    barrier = pltpu.get_barrier_semaphore()
    for peer in greeted:
        pl.semaphore_signal(barrier, inc=1, device_id=peer, device_id_type=MESH)
    pl.semaphore_wait(barrier, len(greeted))

    def remote(src, dst, send, recv, peer):
        return pltpu.make_async_remote_copy(
            src_ref=src, dst_ref=dst, send_sem=send, recv_sem=recv,
            device_id=peer, device_id_type=MESH,
        )

    def row_copy(t, p, way, peer, own=False):
        slot = rows_out.at[pl.ds(t * stripe + p * piece, piece)]
        src = rows_ref.at[pl.ds(p * piece, piece)] if own else slot
        return remote(src, slot, row_send.at[t, p, way], row_recv.at[t, p], peer)

    def go(run, copy):
        if run:
            copy.start()
        else:
            copy.wait_send()

    def arrive(run, t, p):
        if run:
            row_copy(t, p, 0, ((s + 1) % n, m)).wait_recv()

    def up(run, t, p, own=False):
        @pl.when(z < outer - 1)
        def _():
            go(run, row_copy(t, p, 0, (s + inner, m), own))

    def down(run, t, p, own=False):
        @pl.when(z > 0)
        def _():
            go(run, row_copy(t, p, 1, (s - inner, m), own))

    def across(run, t, p, own=False):
        for q in range(1, inner):
            go(run, row_copy(t, p, 1 + q, (z * inner + (xi + q) % inner, m), own))

    def loop(first, body):
        def step(p, carry):
            body(p)
            return carry
        lax.fori_loop(first, pieces, step, 0)

    def own_rows(run):
        def body(p):
            up(run, s, p, True)
            down(run, s, p, True)
            across(run, s, p, True)
        loop(0, body)

    def partner_rows(run):
        if xfirst:
            t = z * inner + (1 - xi)
            for p in range(2):
                arrive(run, t, p)
                up(run, t, p)
                down(run, t, p)

    def hop(run, d):
        def one(p, crossing):
            @pl.when(z >= d)
            def _():
                t = s - d * inner
                arrive(run, t, p)
                up(run, t, p)
                if crossing:
                    across(run, t, p)
                else:
                    t2 = (z - d) * inner + (1 - xi)
                    arrive(run, t2, p)
                    up(run, t2, p)

            @pl.when(z + d < outer)
            def _():
                t = s + d * inner
                arrive(run, t, p)
                down(run, t, p)
                if crossing:
                    across(run, t, p)
                else:
                    t2 = (z + d) * inner + (1 - xi)
                    arrive(run, t2, p)
                    down(run, t2, p)

        if xfirst:
            one(0, False)
            one(1, False)
            loop(2, lambda p: one(p, True))
        else:
            loop(0, lambda p: one(p, True))

    def rest_rows():
        for zz in range(outer):
            for q in range(1, inner):
                t = zz * inner + (xi + q) % inner
                loop(2 if xfirst else 0, lambda p: arrive(True, t, p))

    root_a = s // per
    root_b = (root_a + mp // 2) % mp

    def act_slot(t, h):
        return act_out.at[pl.ds(t * tokens + h * half, half)]

    def act_first(run):
        for j in range(per):
            target = m * per + j

            @pl.when(target != s)
            def _():
                for h, to in ((0, m), (1, opposite)):
                    go(run, remote(
                        act_ref.at[j, pl.ds(h * half, half)], act_slot(s, h),
                        act_send.at[j, h], act_recv.at[s, h], (target, to),
                    ))

            @pl.when(target == s)
            def _():
                for h in range(2):
                    for q, peer in enumerate(mp_peers):
                        go(run, remote(
                            act_ref.at[j, pl.ds(h * half, half)], act_slot(s, h),
                            act_own.at[h, q], act_recv.at[s, h], peer,
                        ))
                mine = pltpu.make_async_copy(
                    act_ref.at[j], act_out.at[pl.ds(s * tokens, tokens)], local_sem.at[1]
                )
                if run:
                    mine.start()
                else:
                    mine.wait()

    def act_wait(t, h):
        remote(act_slot(t, h), act_slot(t, h), act_fwd.at[0, 0], act_recv.at[t, h], mp_peers[0]).wait_recv()

    def act_pass(run):
        for h, root in ((0, root_a), (1, root_b)):
            @pl.when(m == root)
            def _():
                for k in range(1, n):
                    t = (s + k) % n
                    if run:
                        act_wait(t, h)
                    for q, peer in enumerate(mp_peers):
                        go(run, remote(
                            act_slot(t, h), act_slot(t, h), act_fwd.at[t, q], act_recv.at[t, h], peer,
                        ))

    def act_rest():
        for h, root in ((0, root_a), (1, root_b)):
            @pl.when(m != root)
            def _():
                for k in range(1, n):
                    act_wait((s + k) % n, h)

            @pl.when(m != root_a)
            def _():
                act_wait(s, h)

    def sums(run):
        for q, peer in enumerate(mp_peers):
            go(run, remote(terms_ref.at[peer[1]], parts.at[m], rs_send.at[q], rs_recv.at[m], peer))

    def hid_copy(q):
        peer = ((s + q) % n, m)
        return remote(
            outbuf.at[pl.ds(pl.multiple_of(peer[0] * FRAME, FRAME), FRAME)],
            hid_out.at[pl.ds(pl.multiple_of(s * FRAME, FRAME), FRAME)],
            hid_send.at[q], hid_recv.at[s], peer,
        )

    def hid_mine():
        at = pl.ds(pl.multiple_of(s * FRAME, FRAME), FRAME)
        return pltpu.make_async_copy(outbuf.at[at], hid_out.at[at], local_sem.at[2])

    def hidden():
        for q, peer in enumerate(mp_peers):
            remote(terms_ref.at[0], parts.at[peer[1]], rs_send.at[q], rs_recv.at[peer[1]], peer).wait_recv()
        width = parts.shape[2]
        chunk = 256 if width % 256 == 0 else width

        def step(c, carry):
            at = pl.ds(pl.multiple_of(c * chunk, chunk), chunk)
            total = terms_ref[m, :, at].astype(jnp.float32)
            for q in range(1, mp):
                total = total + parts[(m + q) % mp, :, at].astype(jnp.float32)
            outbuf[:, at] = jnp.dot(
                place_ref[...], total.astype(jnp.bfloat16), preferred_element_type=jnp.float32
            ).astype(jnp.bfloat16)
            return carry

        lax.fori_loop(0, width // chunk, step, 0)

    def hid_wait(t):
        at = pl.ds(pl.multiple_of(t * FRAME, FRAME), FRAME)
        remote(outbuf.at[pl.ds(0, FRAME)], hid_out.at[at], hid_send.at[1], hid_recv.at[t], seq_peers[0]).wait_recv()

    def multiply():
        width = terms_ref.shape[2]
        tile = w_buf.shape[1]
        per_part = width // tile

        def where(c):
            return (m + 1 + c // per_part) % mp, (c % per_part) * tile

        def fetch(c, slot):
            q, col = where(c)
            at = pl.ds(pl.multiple_of(q * width + col, tile), tile)
            return pltpu.make_async_copy(w_ref.at[at], w_buf.at[slot], w_sem.at[slot])

        count = mp * per_part
        fetch(0, 0).start()

        def step(c, carry):
            slot = c % 2

            @pl.when(c + 1 < count)
            def _():
                fetch(c + 1, 1 - slot).start()
            fetch(c, slot).wait()
            q, col = where(c)
            terms_ref[q, :, pl.ds(pl.multiple_of(col, tile), tile)] = lax.dot_general(
                rows_ref[...], w_buf[slot], (((1,), (1,)), ((), ())),
                preferred_element_type=jnp.float32,
            ).astype(jnp.bfloat16)
            return carry

        lax.fori_loop(0, count, step, 0)

    keep = pltpu.make_async_copy(rows_ref, rows_out.at[pl.ds(s * stripe, stripe)], local_sem.at[0])
    act_first(True)
    own_rows(True)
    keep.start()
    partner_rows(True)
    multiply()
    sums(True)
    hop(True, 1)
    act_pass(True)
    hidden()
    hop(True, 2)
    for q in range(1, n):
        hid_copy(q).start()
    hid_mine().start()
    for d in range(3, outer):
        hop(True, d)
    rest_rows()
    act_rest()
    for q in range(1, n):
        hid_wait((s + q) % n)

    keep.wait()
    hid_mine().wait()
    own_rows(False)
    sums(False)
    act_first(False)
    partner_rows(False)
    for d in range(1, outer):
        hop(False, d)
    act_pass(False)
    for q in range(1, n):
        hid_copy(q).wait_send()


def exchange(n, mp, tag, rows, acts, place, w_out):
    stripe, quarter = rows.shape
    per, tokens, kept = acts.shape
    width = w_out.shape[0] // mp
    inner = n // 4
    pieces = stripe // 32 if inner == 2 else 1
    vm = pl.BlockSpec(memory_space=pltpu.VMEM)
    anywhere = pl.BlockSpec(memory_space=pl.ANY)
    dma = pltpu.SemaphoreType.DMA
    return pl.pallas_call(
        functools.partial(exchange_kernel, n, mp, inner, pieces),
        out_shape=(
            jax.ShapeDtypeStruct((n * stripe, quarter), jnp.bfloat16),
            jax.ShapeDtypeStruct((n * tokens, kept), jnp.bfloat16),
            jax.ShapeDtypeStruct((n * FRAME, width), jnp.bfloat16),
        ),
        in_specs=[vm] * 3 + [anywhere],
        out_specs=(anywhere,) * 3,
        scratch_shapes=[
            pltpu.VMEM((mp, stripe, width), jnp.bfloat16),
            pltpu.VMEM((mp, stripe, width), jnp.bfloat16),
            pltpu.VMEM((n * FRAME, width), jnp.bfloat16),
            pltpu.VMEM((2, 256 if width % 256 == 0 else width, quarter), jnp.bfloat16),
            dma((2,)),
            dma((mp,)), dma((mp,)),
            dma((n, pieces)), dma((n, pieces, 1 + inner)),
            dma((n, 2)), dma((per, 2)), dma((n, mp)), dma((2, mp)),
            dma((n,)), dma((n,)), dma((3,)),
        ],
        compiler_params=pltpu.CompilerParams(
            collective_id=tag, has_side_effects=True, vmem_limit_bytes=60 * 1024 * 1024
        ),
    )(rows, acts, place, w_out)


def spread(counts, before, base, size):
    r = jnp.arange(size, dtype=jnp.int32)
    inside = (r >= before[..., None]) & (r < (before + counts)[..., None])
    return jnp.sum(jnp.where(inside, (base - before)[..., None] + r + 1, 0), axis=-2) - 1


def local(n, mp, grad_rows, img_start, img_len, img_owner, pre_act, w_out):
    stripe, quarter = grad_rows.shape
    width = pre_act.shape[1]
    kept = w_out.shape[0] // n
    frames = stripe // FRAME
    here = lax.axis_index("seq")
    owner = img_owner.reshape(n, frames)
    starts = img_start.reshape(n, frames)
    lengths = img_len.reshape(n, frames)
    before = jnp.cumsum(lengths, axis=1) - lengths
    row = jnp.arange(FRAME, dtype=jnp.int32)
    column = jnp.arange(stripe, dtype=jnp.int32)

    values = pre_act.astype(jnp.float32)
    activation, derivative = gelu_parts(values)
    activation = activation.astype(jnp.bfloat16)
    acts = activation.reshape(stripe, width // kept, kept).transpose(1, 0, 2)

    my_owner = lax.dynamic_slice_in_dim(owner, here, 1)[0]
    my_start = lax.dynamic_slice_in_dim(starts, here, 1)[0] - here * stripe
    my_length = lax.dynamic_slice_in_dim(lengths, here, 1)[0]
    my_before = lax.dynamic_slice_in_dim(before, here, 1)[0]
    to = (my_owner[None, :] == jnp.arange(n, dtype=jnp.int32)[:, None]).astype(jnp.int32)
    first = jnp.sum(to * my_before[None, :], axis=1)
    count = jnp.sum(to * my_length[None, :], axis=1)
    at = jnp.where(row[None, :] < count[:, None], first[:, None] + row[None, :], -1).reshape(n * FRAME, 1)
    order = img_owner * frames + jnp.arange(n * frames, dtype=jnp.int32) % frames
    factor = 1.0 / math.sqrt(n * stripe)

    def with_size(tag, size, grad_rows, acts, w_out):
        source = spread(my_length, my_before, my_start, size)
        live = (source[:, None] == column[None, :]).astype(jnp.bfloat16)
        rows = jnp.dot(live, grad_rows, preferred_element_type=jnp.float32).astype(jnp.bfloat16)
        place = (at == jnp.arange(size, dtype=jnp.int32)[None, :]).astype(jnp.bfloat16)
        rows_all, act_all, hid = exchange(n, mp, tag, rows, acts, place, w_out)
        blocks = act_all.reshape(n * frames, FRAME, kept)[order].reshape(n, stripe, kept)
        block = jnp.broadcast_to(jnp.arange(frames, dtype=jnp.int32) * FRAME, (n, frames))
        taken = spread(lengths, before, block, size)
        lined = (taken[:, :, None] == column[None, None, :]).astype(jnp.bfloat16)
        act_rows = jnp.einsum(
            "trc,tck->trk", lined, blocks, preferred_element_type=jnp.float32
        ).astype(jnp.bfloat16).reshape(n * size, kept)
        product = lax.dot_general(
            act_rows, rows_all, (((0,), (0,)), ((), ())), preferred_element_type=jnp.float32
        ) * factor
        return lax.optimization_barrier(product.astype(jnp.bfloat16)), hid

    sizes = [stripe // 16 * k for k in (12, 13, 16)]
    most = jnp.max(jnp.sum(lengths, axis=1))
    which = sum((most > size).astype(jnp.int32) for size in sizes[:-1])
    weight_grad, hid = lax.switch(
        which,
        [functools.partial(with_size, tag, size) for tag, size in enumerate(sizes)],
        grad_rows, acts, w_out,
    )

    came = jnp.arange(n * FRAME, dtype=jnp.int32)
    from_me = (owner == here).T
    pick = jnp.repeat(jnp.repeat(from_me, FRAME, axis=0), FRAME, axis=1)
    pick = (pick & (column[:, None] % FRAME == came[None, :] % FRAME)).astype(jnp.bfloat16)
    hidden_grad = jnp.dot(pick, hid, preferred_element_type=jnp.float32)
    pre_grad = (hidden_grad * derivative).astype(jnp.bfloat16)
    return (pre_grad, weight_grad)


def fused_kernel(
    n, mp, inner, pieces, early, factor,
    order_ref, rows_ref, act_ref, place_ref, taken_ref, w_ref,
    hid_out, grad_out,
    rows_all, act_all, relay, w_all, acc, hot, block, lined, picked, terms, parts, hid, stage,
    w_sem, rs_recv, rs_send, row_recv, row_send, act_recv, act_send, act_fwd, act_own,
    relay_recv, relay_send, relay_fwd, far_recv, far_send, local_sem, out_sem,
):
    s = lax.axis_index("seq")
    m = lax.axis_index("mp")
    outer = n // inner
    low = outer // 2
    z, xi = s // inner, s % inner
    size = rows_ref.shape[0]
    piece = size // pieces
    per, frames, _, kept = act_ref.shape
    half = frames // 2
    quarter = rows_ref.shape[1]
    width = parts.shape[1]
    pair = inner * FRAME
    edge = (z == 0) | (z == outer - 1)
    sibling = m + 1 - 2 * (m % 2)
    opposite = (m + mp // 2) % mp
    seq_peers = [((s + q) % n, m) for q in range(1, n)]
    mp_peers = [(s, (m + q) % mp) for q in range(1, mp)]
    greeted = seq_peers + mp_peers
    barrier = pltpu.get_barrier_semaphore()
    for peer in greeted:
        pl.semaphore_signal(barrier, inc=1, device_id=peer, device_id_type=MESH)
    pl.semaphore_wait(barrier, len(greeted))

    def remote(src, dst, send, recv, peer):
        return pltpu.make_async_remote_copy(
            src_ref=src, dst_ref=dst, send_sem=send, recv_sem=recv,
            device_id=peer, device_id_type=MESH,
        )

    def go(run, copy):
        if run:
            copy.start()
        else:
            copy.wait_send()

    def loop(first, last, body):
        def step(p, carry):
            body(p)
            return carry
        lax.fori_loop(first, last, step, 0)

    def layer_of(k):
        mate = jnp.where(z < low, low - 1 - z, 3 * low - 1 - z)
        return jnp.where(k == 0, z, jnp.where(k == 1, mate, jnp.where(z < low, k, outer - 1 - k)))

    def row_copy(t, p, way, peer, own=False):
        slot = rows_all.at[t // inner, pl.ds((t % inner) * size + p * piece, piece)]
        src = rows_ref.at[pl.ds(p * piece, piece)] if own else slot
        return remote(src, slot, row_send.at[t, p, way], row_recv.at[t, p], peer)

    def arrive(run, t, p):
        if run:
            row_copy(t, p, 0, ((s + 1) % n, m)).wait_recv()

    def up(run, t, p, own=False):
        @pl.when(z < outer - 1)
        def _():
            go(run, row_copy(t, p, 0, (s + inner, m), own))

    def down(run, t, p, own=False):
        @pl.when(z > 0)
        def _():
            go(run, row_copy(t, p, 1, (s - inner, m), own))

    def across(run, t, p, own=False):
        go(run, row_copy(t, p, 2, (z * inner + 1 - xi, m), own))

    def own_rows(run, first, last):
        def body(p):
            up(run, s, p, True)
            down(run, s, p, True)
            across(run, s, p, True)
        loop(first, last, body)

    def partner_row(run, p):
        t = z * inner + (1 - xi)
        arrive(run, t, p)
        up(run, t, p)
        down(run, t, p)

    def hop(run, d, first, last):
        def one(p):
            @pl.when(edge & (d == 1) & (p >= early))
            def _():
                partner_row(run, p)

            @pl.when(z >= d)
            def _():
                t = s - d * inner
                arrive(run, t, p)
                up(run, t, p)

                @pl.when((p >= early) & ((d > 1) | (z > 1)))
                def _():
                    across(run, t, p)

                @pl.when(p < early)
                def _():
                    t2 = (z - d) * inner + (1 - xi)
                    arrive(run, t2, p)
                    up(run, t2, p)

            @pl.when(z + d < outer)
            def _():
                t = s + d * inner
                arrive(run, t, p)
                down(run, t, p)

                @pl.when((p >= early) & ((d > 1) | (z < outer - 2)))
                def _():
                    across(run, t, p)

                @pl.when(p < early)
                def _():
                    t2 = (z + d) * inner + (1 - xi)
                    arrive(run, t2, p)
                    down(run, t2, p)
        loop(first, last, one)

    def rest(k):
        t = layer_of(k) * inner + (1 - xi)

        @pl.when((k > 0) | jnp.logical_not(edge))
        def _():
            loop(early, pieces, lambda p: arrive(True, t, p))

    root_a = s // per
    root_b = (root_a + mp // 2) % mp

    def act_slot(t, h):
        return act_all.at[pl.ds(t * frames + h * half, half)]

    def act_piece(j, h):
        return act_ref.at[j, pl.ds(h * half, half)]

    def act_mine():
        return pltpu.make_async_copy(
            act_ref.at[xi], act_all.at[pl.ds(s * frames, frames)], local_sem.at[1]
        )

    def act_first(run):
        for j in range(per):
            target = m * per + j

            @pl.when(target != s)
            def _():
                go(run, remote(
                    act_piece(j, 1), relay.at[j], relay_send.at[j], relay_recv.at[j], (s, opposite)
                ))
                go(run, remote(
                    act_piece(j, 0), act_slot(s, 0), act_send.at[j], act_recv.at[s, 0], (target, m)
                ))

            @pl.when(target == s)
            def _():
                for h in range(2):
                    for q, to in enumerate((opposite, sibling)):
                        go(run, remote(
                            act_piece(j, h), act_slot(s, h), act_own.at[h, q], act_recv.at[s, h], (s, to)
                        ))
                if run:
                    act_mine().start()

    def act_relay(run):
        for j in range(per):
            target = opposite * per + j

            @pl.when(target != s)
            def _():
                if run:
                    remote(
                        relay.at[j], relay.at[j], relay_send.at[j], relay_recv.at[j], (s, opposite)
                    ).wait_recv()
                go(run, remote(
                    relay.at[j], act_slot(s, 1), relay_fwd.at[j], act_recv.at[s, 1], (target, m)
                ))

    def act_wait(t, h):
        remote(act_slot(t, h), act_slot(t, h), act_fwd.at[0, 0, 0], act_recv.at[t, h], mp_peers[0]).wait_recv()

    def act_send_on(run, t, h, to, q):
        go(run, remote(
            act_slot(t, h), act_slot(t, h), act_fwd.at[t, h, q], act_recv.at[t, h], (s, to)
        ))

    def act_pass(run):
        def others(body):
            def step(i):
                t = layer_of(i // inner) * inner + i % inner

                @pl.when(t != s)
                def _():
                    body(t)
            loop(0, n, step)

        for h, root in ((0, root_a), (1, root_b)):
            @pl.when(m == root)
            def _():
                def first(t):
                    if run:
                        act_wait(t, h)
                    act_send_on(run, t, h, opposite, 0)
                    act_send_on(run, t, h, sibling, 1)
                others(first)

                def second(t):
                    if run:
                        act_wait(t, 1 - h)
                    act_send_on(run, t, 1 - h, sibling, 1)
                others(second)

        @pl.when(m == root_b)
        def _():
            for h in range(2):
                if run:
                    act_wait(s, h)
                act_send_on(run, s, h, sibling, 1)

    def act_rest():
        @pl.when((m != root_a) & (m != root_b))
        def _():
            def step(t):
                for h in range(2):
                    act_wait(t, h)
            loop(0, n, step)

        @pl.when(m == root_a)
        def _():
            act_mine().wait()

    def part_copy(run, i, q):
        go(run, remote(
            terms.at[i % 2, mp_peers[q][1]], parts.at[i * mp + m], rs_send.at[i, q], rs_recv.at[i, m], mp_peers[q],
        ))

    def source(i, j):
        return jnp.where(
            edge,
            jnp.where(i == 0, s, layer_of(jnp.maximum(i - 1, 0)) * inner + j),
            layer_of(i) * inner + j,
        )

    def hidden(i):
        @pl.when(i >= 2)
        def _():
            for q in range(mp - 1):
                part_copy(False, i - 2, q)
        tile = 256 if quarter % 256 == 0 else quarter

        def choose(c):
            at = pl.ds(pl.multiple_of(c * tile, tile), tile)
            found = []
            for j in range(inner):
                t = source(i, j)
                rows = rows_all[t // inner, pl.ds(pl.multiple_of((t % inner) * size, 16), size), at]
                found.append(jnp.dot(
                    place_ref[pl.ds(pl.multiple_of((i * inner + j) * FRAME, FRAME), FRAME), :],
                    rows, preferred_element_type=jnp.float32,
                ))
            picked[at, :] = jnp.concatenate(found, axis=0).T.astype(jnp.bfloat16)
        loop(0, quarter // tile, choose)
        block_rows = 256 if width % 256 == 0 else width
        for q in range(mp):
            to = (m + 1 + q) % mp

            def step(c):
                col = pl.multiple_of(c * block_rows, block_rows)
                value = jnp.dot(
                    w_all[pl.ds(pl.multiple_of(to * width + c * block_rows, block_rows), block_rows), :],
                    picked[...], preferred_element_type=jnp.float32,
                ).astype(jnp.bfloat16)
                if q < mp - 1:
                    terms[i % 2, to, pl.ds(col, block_rows), :] = value
                else:
                    parts[i * mp + m, pl.ds(col, block_rows), :] = value
            loop(0, width // block_rows, step)
            if q > 0:
                part_copy(True, i, q - 1)

    def reduce(i):
        for q, peer in enumerate(mp_peers):
            remote(
                terms.at[0, 0], parts.at[i * mp + peer[1]], rs_send.at[i, q], rs_recv.at[i, peer[1]], peer
            ).wait_recv()
        tile = 256 if width % 256 == 0 else width

        def step(c):
            at = pl.ds(pl.multiple_of(c * tile, tile), tile)
            total = parts[i * mp, at, :].astype(jnp.float32)
            for q in range(1, mp):
                total = total + parts[i * mp + q, at, :].astype(jnp.float32)
            total = total.T.astype(jnp.bfloat16)
            for j in range(inner):
                t = jnp.where(edge & (i == 0), n + j, source(i, j))
                hid[t, :, at] = total[j * FRAME:(j + 1) * FRAME]
        loop(0, width // tile, step)

        @pl.when(edge & (i == 0))
        def _():
            far(True)

    def far(run):
        for j in range(inner):
            go(run, remote(
                hid.at[n + j], hid.at[s], far_send.at[j], far_recv.at[xi],
                ((outer - 1 - z) * inner + j, m),
            ))

    def far_wait():
        for j in range(inner):
            t = (outer - 1 - z) * inner + j
            remote(hid.at[t], hid.at[t], far_send.at[j], far_recv.at[j], seq_peers[0]).wait_recv()

    def line_up(k):
        layer = layer_of(k)
        for j in range(inner):
            t = layer * inner + j

            def frame(f):
                at = pl.ds(pl.multiple_of(f * FRAME, FRAME), FRAME)
                block[at, :] = act_all[order_ref[t * frames + f]]
                row = lax.broadcasted_iota(jnp.int32, (FRAME, size), 0) + f * FRAME
                hot[at, :] = jnp.where(row == taken_ref[t], 1.0, 0.0).astype(jnp.bfloat16)
            loop(0, frames, frame)

            def step(c):
                at = pl.ds(pl.multiple_of(c * 128, 128), 128)
                lined[k % 2, at, pl.ds(j * size, size)] = lax.dot_general(
                    block[:, at], hot[...], (((0,), (0,)), ((), ())),
                    preferred_element_type=jnp.float32,
                ).astype(jnp.bfloat16)
            loop(0, kept // 128, step)

    def weights(k):
        layer = layer_of(k)
        tile = 256 if quarter % 256 == 0 else quarter
        count = quarter // tile

        def put(c, slot):
            at = pl.ds(pl.multiple_of(c * tile, tile), tile)
            return pltpu.make_async_copy(stage.at[slot], grad_out.at[:, at], out_sem.at[slot])

        def step(c):
            at = pl.ds(pl.multiple_of(c * tile, tile), tile)
            value = acc[:, at] + jnp.dot(
                lined[k % 2], rows_all[layer, :, at], preferred_element_type=jnp.float32
            )

            @pl.when(k < outer - 1)
            def _():
                acc[:, at] = value

            @pl.when(k == outer - 1)
            def _():
                slot = c % 2

                @pl.when(c > 1)
                def _():
                    put(c - 2, slot).wait()
                stage[slot] = (value * factor).astype(jnp.bfloat16)
                put(c, slot).start()
        loop(0, count, step)

        @pl.when(k < outer - 1)
        def _():
            line_up(k + 1)

        @pl.when(k == outer - 1)
        def _():
            for c in range(max(0, count - 2), count):
                put(c, c % 2).wait()

    def clear(c):
        at = pl.ds(pl.multiple_of(c * 128, 128), 128)
        acc[at, :] = jnp.zeros((128, quarter), jnp.float32)

    fetch = pltpu.make_async_copy(w_ref, w_all, w_sem)
    keep = pltpu.make_async_copy(
        rows_ref, rows_all.at[z, pl.ds(xi * size, size)], local_sem.at[0]
    )
    lead = min(4, pieces)
    act_first(True)
    own_rows(True, 0, lead)
    keep.start()
    fetch.start()
    act_relay(True)
    own_rows(True, lead, pieces)
    loop(0, kept // 128, clear)
    loop(0, early, lambda p: partner_row(True, p))
    act_pass(True)
    keep.wait()
    fetch.wait()

    def since(e, *steps):
        total = 0
        for at in steps:
            total = total + jnp.where(e >= at, 1, 0)
        return total

    middle = pieces // 2

    def stage_of(e):
        late = e % 2
        hop(True, 1 + e // 2, late * middle, jnp.where(late == 1, pieces, middle))
        terms_from, terms_to = since(e, 1, 3, 4, 5), since(e, 0, 2, 3, 4)
        grad_from, grad_to = since(e, 2, 4, 5, 6), since(e, 1, 3, 4, 5)
        loop(jnp.where(edge, grad_from, terms_from), jnp.where(edge, grad_to, terms_to), rest)
        loop(since(e, 3, 4, 6, 6), since(e, 2, 3, 5, 5), reduce)
        loop(terms_from, terms_to, hidden)

        @pl.when(e == 1)
        def _():
            act_rest()
            line_up(0)
        loop(grad_from, grad_to, weights)

    loop(0, 2 * (outer - 1), stage_of)

    @pl.when(edge)
    def _():
        far_wait()
    for f in range(frames):
        hid_out[pl.ds(f * FRAME, FRAME), :] = hid[order_ref[n * frames + f]]

    act_first(False)
    act_relay(False)
    own_rows(False, 0, pieces)
    for i in range(outer - 2, outer):
        for q in range(mp - 1):
            part_copy(False, i, q)
    loop(0, early, lambda p: partner_row(False, p))
    loop(1, outer, lambda d: hop(False, d, 0, pieces))
    act_pass(False)

    @pl.when(edge)
    def _():
        far(False)


def fused(n, mp, grain, early, tag, factor, order, rows, acts, place, taken, w_out):
    stripe, quarter = rows.shape
    per, frames, _, kept = acts.shape
    width = w_out.shape[0] // mp
    inner = n // 4
    outer = n // inner
    pieces = stripe // grain
    vm = pl.BlockSpec(memory_space=pltpu.VMEM)
    anywhere = pl.BlockSpec(memory_space=pl.ANY)
    dma = pltpu.SemaphoreType.DMA
    b16 = jnp.bfloat16
    return pl.pallas_call(
        functools.partial(fused_kernel, n, mp, inner, pieces, early, factor),
        out_shape=(
            jax.ShapeDtypeStruct((frames * FRAME, width), b16),
            jax.ShapeDtypeStruct((kept, quarter), b16),
        ),
        in_specs=[pl.BlockSpec(memory_space=pltpu.SMEM), anywhere, anywhere, vm, vm, anywhere],
        out_specs=(vm, anywhere),
        scratch_shapes=[
            pltpu.VMEM((outer, inner * stripe, quarter), b16),
            pltpu.VMEM((n * frames, FRAME, kept), b16),
            pltpu.VMEM((per, frames // 2, FRAME, kept), b16),
            pltpu.VMEM(w_out.shape, b16),
            pltpu.VMEM((kept, quarter), jnp.float32),
            pltpu.VMEM((frames * FRAME, stripe), b16),
            pltpu.VMEM((frames * FRAME, kept), b16),
            pltpu.VMEM((2, kept, inner * stripe), b16),
            pltpu.VMEM((quarter, inner * FRAME), b16),
            pltpu.VMEM((2, mp, width, inner * FRAME), b16),
            pltpu.VMEM((outer * mp, width, inner * FRAME), b16),
            pltpu.VMEM((n + inner, FRAME, width), b16),
            pltpu.VMEM((2, kept, 256 if quarter % 256 == 0 else quarter), b16),
            dma(()), dma((outer, mp)), dma((outer, mp)),
            dma((n, pieces)), dma((n, pieces, 3)),
            dma((n, 2)), dma((per,)), dma((n, 2, 2)), dma((2, 2)),
            dma((per,)), dma((per,)), dma((per,)), dma((inner,)), dma((inner,)),
            dma((2,)), dma((2,)),
        ],
        compiler_params=pltpu.CompilerParams(
            collective_id=tag, has_side_effects=True, vmem_limit_bytes=67043328
        ),
    )(order, rows, acts, place, taken, w_out)


GRAIN, EARLY = 32, 1


def local_fused(n, mp, grad_rows, img_start, img_len, img_owner, pre_act, w_out):
    stripe, quarter = grad_rows.shape
    width = pre_act.shape[1]
    kept = w_out.shape[0] // n
    frames = stripe // FRAME
    per = width // kept
    here = lax.axis_index("seq")
    owner = img_owner.reshape(n, frames)
    starts = img_start.reshape(n, frames)
    lengths = img_len.reshape(n, frames)
    before = jnp.cumsum(lengths, axis=1) - lengths
    row = jnp.arange(FRAME, dtype=jnp.int32)
    column = jnp.arange(stripe, dtype=jnp.int32)

    values = pre_act.astype(jnp.float32)
    activation, derivative = gelu_parts(values)
    activation = activation.astype(jnp.bfloat16)
    acts = activation.reshape(stripe, per, kept).transpose(1, 0, 2).reshape(per, frames, FRAME, kept)

    my_start = lax.dynamic_slice_in_dim(starts, here, 1)[0] - here * stripe
    my_length = lax.dynamic_slice_in_dim(lengths, here, 1)[0]
    my_before = lax.dynamic_slice_in_dim(before, here, 1)[0]
    inner, outer = n // 4, 4
    z = here // inner
    edge = (z == 0) | (z == outer - 1)
    step = jnp.arange(n, dtype=jnp.int32) // inner
    side = jnp.arange(n, dtype=jnp.int32) % inner
    k = jnp.where(edge, jnp.maximum(step - 1, 0), step)
    mate = jnp.where(z < outer // 2, outer // 2 - 1 - z, 3 * outer // 2 - 1 - z)
    layer = jnp.where(k == 0, z, jnp.where(k == 1, mate, jnp.where(z < outer // 2, k, outer - 1 - k)))
    distant = edge & (step == 0)
    from_stripe = jnp.where(distant, here, layer * inner + side)
    to_owner = jnp.where(distant, (outer - 1 - z) * inner + side, here)
    mine = (owner == here).astype(jnp.int32)
    match = (from_stripe[:, None, None] == jnp.arange(n, dtype=jnp.int32)[None, :, None])
    match = (match & (owner[None] == to_owner[:, None, None])).astype(jnp.int32)
    first = jnp.sum(match * before[None], axis=(1, 2))
    count = jnp.sum(match * lengths[None], axis=(1, 2))
    at = jnp.where(row[None, :] < count[:, None], first[:, None] + row[None, :], -1).reshape(n * FRAME, 1)
    source_of = jnp.sum(mine * jnp.arange(n, dtype=jnp.int32)[:, None], axis=0)
    order = img_owner * frames + jnp.arange(n * frames, dtype=jnp.int32) % frames
    order = jnp.concatenate([order, source_of])
    factor = 1.0 / math.sqrt(n * stripe)
    block = jnp.broadcast_to(jnp.arange(frames, dtype=jnp.int32) * FRAME, (n, frames))

    def with_size(tag, size, grad_rows, acts, w_out):
        source = spread(my_length, my_before, my_start, size)
        live = (source[:, None] == column[None, :]).astype(jnp.bfloat16)
        rows = jnp.dot(live, grad_rows, preferred_element_type=jnp.float32).astype(jnp.bfloat16)
        place = (at == jnp.arange(size, dtype=jnp.int32)[None, :]).astype(jnp.bfloat16)
        taken = spread(lengths, before, block, size).reshape(n, 1, size)
        return fused(n, mp, GRAIN, EARLY, tag, factor, order, rows, acts, place, taken, w_out)

    sizes = [stripe // 16 * k for k in (12, 13, 16)]
    most = jnp.max(jnp.sum(lengths, axis=1))
    which = sum((most > size).astype(jnp.int32) for size in sizes[:-1])
    hid, weight_grad = lax.switch(
        which,
        [functools.partial(with_size, tag, size) for tag, size in enumerate(sizes)],
        grad_rows, acts, w_out,
    )
    pre_grad = (hid.astype(jnp.float32) * derivative).astype(jnp.bfloat16)
    return (pre_grad, weight_grad)


def chosen(n, mp, grad_rows, *rest):
    whole = n * grad_rows.shape[0] * grad_rows.shape[1] + rest[-1].shape[0] * rest[-1].shape[1]
    fits = n * FRAME == grad_rows.shape[0] and n == 2 * mp and 2 * whole <= 40 * 1024 * 1024
    return (local_fused if fits else local)(n, mp, grad_rows, *rest)


def solution(mesh):
    return jax.shard_map(
        functools.partial(chosen, mesh.shape["seq"], mesh.shape["mp"]),
        mesh=mesh,
        in_specs=(P("seq", "mp"), P(), P(), P(), P("seq", "mp"), P(None, "mp")),
        out_specs=(P("seq", "mp"), P("seq", "mp")),
        check_vma=False,
    )
```

```python
import functools
import math

import jax
import jax.numpy as jnp
from jax import lax
from jax.experimental import pallas as pl
from jax.experimental.pallas import tpu as pltpu
from jax.sharding import PartitionSpec as P

FRAME = 64
MESH = pl.DeviceIdType.MESH


def gelu_parts(values):
    normal_cdf = 0.5 * (1.0 + lax.erf(values * 0.7071067811865476))
    density = jnp.exp(-0.5 * values * values) * 0.3989422804014327
    return (values * normal_cdf, normal_cdf + values * density)


def exchange_kernel(
    n, mp, inner, pieces,
    rows_ref, act_ref, place_ref, w_ref,
    rows_out, act_out, hid_out,
    terms_ref, parts, outbuf, w_buf, w_sem,
    rs_recv, rs_send, row_recv, row_send, act_recv, act_send, act_fwd, act_own,
    hid_recv, hid_send, local_sem,
):
    s = lax.axis_index("seq")
    m = lax.axis_index("mp")
    outer = n // inner
    z, xi = s // inner, s % inner
    stripe = rows_ref.shape[0]
    piece = stripe // pieces
    tokens = act_ref.shape[1]
    half = tokens // 2
    per = act_ref.shape[0]
    xfirst = inner == 2
    seq_peers = [((s + q) % n, m) for q in range(1, n)]
    mp_peers = [(s, (m + q) % mp) for q in range(1, mp)]

    opposite = (m + mp // 2) % mp
    greeted = seq_peers + mp_peers + [((s + q) % n, opposite) for q in range(1, n)]
    barrier = pltpu.get_barrier_semaphore()
    for peer in greeted:
        pl.semaphore_signal(barrier, inc=1, device_id=peer, device_id_type=MESH)
    pl.semaphore_wait(barrier, len(greeted))

    def remote(src, dst, send, recv, peer):
        return pltpu.make_async_remote_copy(
            src_ref=src, dst_ref=dst, send_sem=send, recv_sem=recv,
            device_id=peer, device_id_type=MESH,
        )

    def row_copy(t, p, way, peer, own=False):
        slot = rows_out.at[pl.ds(t * stripe + p * piece, piece)]
        src = rows_ref.at[pl.ds(p * piece, piece)] if own else slot
        return remote(src, slot, row_send.at[t, p, way], row_recv.at[t, p], peer)

    def go(run, copy):
        if run:
            copy.start()
        else:
            copy.wait_send()

    def arrive(run, t, p):
        if run:
            row_copy(t, p, 0, ((s + 1) % n, m)).wait_recv()

    def up(run, t, p, own=False):
        @pl.when(z < outer - 1)
        def _():
            go(run, row_copy(t, p, 0, (s + inner, m), own))

    def down(run, t, p, own=False):
        @pl.when(z > 0)
        def _():
            go(run, row_copy(t, p, 1, (s - inner, m), own))

    def across(run, t, p, own=False):
        for q in range(1, inner):
            go(run, row_copy(t, p, 1 + q, (z * inner + (xi + q) % inner, m), own))

    def loop(first, body):
        def step(p, carry):
            body(p)
            return carry
        lax.fori_loop(first, pieces, step, 0)

    def own_rows(run):
        def body(p):
            up(run, s, p, True)
            down(run, s, p, True)
            across(run, s, p, True)
        loop(0, body)

    def partner_rows(run):
        if xfirst:
            t = z * inner + (1 - xi)
            for p in range(2):
                arrive(run, t, p)
                up(run, t, p)
                down(run, t, p)

    def hop(run, d):
        def one(p, crossing):
            @pl.when(z >= d)
            def _():
                t = s - d * inner
                arrive(run, t, p)
                up(run, t, p)
                if crossing:
                    across(run, t, p)
                else:
                    t2 = (z - d) * inner + (1 - xi)
                    arrive(run, t2, p)
                    up(run, t2, p)

            @pl.when(z + d < outer)
            def _():
                t = s + d * inner
                arrive(run, t, p)
                down(run, t, p)
                if crossing:
                    across(run, t, p)
                else:
                    t2 = (z + d) * inner + (1 - xi)
                    arrive(run, t2, p)
                    down(run, t2, p)

        if xfirst:
            one(0, False)
            one(1, False)
            loop(2, lambda p: one(p, True))
        else:
            loop(0, lambda p: one(p, True))

    def rest_rows():
        for zz in range(outer):
            for q in range(1, inner):
                t = zz * inner + (xi + q) % inner
                loop(2 if xfirst else 0, lambda p: arrive(True, t, p))

    root_a = s // per
    root_b = (root_a + mp // 2) % mp

    def act_slot(t, h):
        return act_out.at[pl.ds(t * tokens + h * half, half)]

    def act_first(run):
        for j in range(per):
            target = m * per + j

            @pl.when(target != s)
            def _():
                for h, to in ((0, m), (1, opposite)):
                    go(run, remote(
                        act_ref.at[j, pl.ds(h * half, half)], act_slot(s, h),
                        act_send.at[j, h], act_recv.at[s, h], (target, to),
                    ))

            @pl.when(target == s)
            def _():
                for h in range(2):
                    for q, peer in enumerate(mp_peers):
                        go(run, remote(
                            act_ref.at[j, pl.ds(h * half, half)], act_slot(s, h),
                            act_own.at[h, q], act_recv.at[s, h], peer,
                        ))
                mine = pltpu.make_async_copy(
                    act_ref.at[j], act_out.at[pl.ds(s * tokens, tokens)], local_sem.at[1]
                )
                if run:
                    mine.start()
                else:
                    mine.wait()

    def act_wait(t, h):
        remote(act_slot(t, h), act_slot(t, h), act_fwd.at[0, 0], act_recv.at[t, h], mp_peers[0]).wait_recv()

    def act_pass(run):
        for h, root in ((0, root_a), (1, root_b)):
            @pl.when(m == root)
            def _():
                for k in range(1, n):
                    t = (s + k) % n
                    if run:
                        act_wait(t, h)
                    for q, peer in enumerate(mp_peers):
                        go(run, remote(
                            act_slot(t, h), act_slot(t, h), act_fwd.at[t, q], act_recv.at[t, h], peer,
                        ))

    def act_rest():
        for h, root in ((0, root_a), (1, root_b)):
            @pl.when(m != root)
            def _():
                for k in range(1, n):
                    act_wait((s + k) % n, h)

            @pl.when(m != root_a)
            def _():
                act_wait(s, h)

    def sums(run):
        for q, peer in enumerate(mp_peers):
            go(run, remote(terms_ref.at[peer[1]], parts.at[m], rs_send.at[q], rs_recv.at[m], peer))

    def hid_copy(q):
        peer = ((s + q) % n, m)
        return remote(
            outbuf.at[pl.ds(pl.multiple_of(peer[0] * FRAME, FRAME), FRAME)],
            hid_out.at[pl.ds(pl.multiple_of(s * FRAME, FRAME), FRAME)],
            hid_send.at[q], hid_recv.at[s], peer,
        )

    def hid_mine():
        at = pl.ds(pl.multiple_of(s * FRAME, FRAME), FRAME)
        return pltpu.make_async_copy(outbuf.at[at], hid_out.at[at], local_sem.at[2])

    def hidden():
        for q, peer in enumerate(mp_peers):
            remote(terms_ref.at[0], parts.at[peer[1]], rs_send.at[q], rs_recv.at[peer[1]], peer).wait_recv()
        width = parts.shape[2]
        chunk = 256 if width % 256 == 0 else width

        def step(c, carry):
            at = pl.ds(pl.multiple_of(c * chunk, chunk), chunk)
            total = terms_ref[m, :, at].astype(jnp.float32)
            for q in range(1, mp):
                total = total + parts[(m + q) % mp, :, at].astype(jnp.float32)
            outbuf[:, at] = jnp.dot(
                place_ref[...], total.astype(jnp.bfloat16), preferred_element_type=jnp.float32
            ).astype(jnp.bfloat16)
            return carry

        lax.fori_loop(0, width // chunk, step, 0)

    def hid_wait(t):
        at = pl.ds(pl.multiple_of(t * FRAME, FRAME), FRAME)
        remote(outbuf.at[pl.ds(0, FRAME)], hid_out.at[at], hid_send.at[1], hid_recv.at[t], seq_peers[0]).wait_recv()

    def multiply():
        width = terms_ref.shape[2]
        tile = w_buf.shape[1]
        per_part = width // tile

        def where(c):
            return (m + 1 + c // per_part) % mp, (c % per_part) * tile

        def fetch(c, slot):
            q, col = where(c)
            at = pl.ds(pl.multiple_of(q * width + col, tile), tile)
            return pltpu.make_async_copy(w_ref.at[at], w_buf.at[slot], w_sem.at[slot])

        count = mp * per_part
        fetch(0, 0).start()

        def step(c, carry):
            slot = c % 2

            @pl.when(c + 1 < count)
            def _():
                fetch(c + 1, 1 - slot).start()
            fetch(c, slot).wait()
            q, col = where(c)
            terms_ref[q, :, pl.ds(pl.multiple_of(col, tile), tile)] = lax.dot_general(
                rows_ref[...], w_buf[slot], (((1,), (1,)), ((), ())),
                preferred_element_type=jnp.float32,
            ).astype(jnp.bfloat16)
            return carry

        lax.fori_loop(0, count, step, 0)

    keep = pltpu.make_async_copy(rows_ref, rows_out.at[pl.ds(s * stripe, stripe)], local_sem.at[0])
    act_first(True)
    own_rows(True)
    keep.start()
    partner_rows(True)
    multiply()
    sums(True)
    hop(True, 1)
    act_pass(True)
    hidden()
    hop(True, 2)
    for q in range(1, n):
        hid_copy(q).start()
    hid_mine().start()
    for d in range(3, outer):
        hop(True, d)
    rest_rows()
    act_rest()
    for q in range(1, n):
        hid_wait((s + q) % n)

    keep.wait()
    hid_mine().wait()
    own_rows(False)
    sums(False)
    act_first(False)
    partner_rows(False)
    for d in range(1, outer):
        hop(False, d)
    act_pass(False)
    for q in range(1, n):
        hid_copy(q).wait_send()


def exchange(n, mp, tag, rows, acts, place, w_out):
    stripe, quarter = rows.shape
    per, tokens, kept = acts.shape
    width = w_out.shape[0] // mp
    inner = n // 4
    pieces = stripe // 32 if inner == 2 else 1
    vm = pl.BlockSpec(memory_space=pltpu.VMEM)
    anywhere = pl.BlockSpec(memory_space=pl.ANY)
    dma = pltpu.SemaphoreType.DMA
    return pl.pallas_call(
        functools.partial(exchange_kernel, n, mp, inner, pieces),
        out_shape=(
            jax.ShapeDtypeStruct((n * stripe, quarter), jnp.bfloat16),
            jax.ShapeDtypeStruct((n * tokens, kept), jnp.bfloat16),
            jax.ShapeDtypeStruct((n * FRAME, width), jnp.bfloat16),
        ),
        in_specs=[vm] * 3 + [anywhere],
        out_specs=(anywhere,) * 3,
        scratch_shapes=[
            pltpu.VMEM((mp, stripe, width), jnp.bfloat16),
            pltpu.VMEM((mp, stripe, width), jnp.bfloat16),
            pltpu.VMEM((n * FRAME, width), jnp.bfloat16),
            pltpu.VMEM((2, 256 if width % 256 == 0 else width, quarter), jnp.bfloat16),
            dma((2,)),
            dma((mp,)), dma((mp,)),
            dma((n, pieces)), dma((n, pieces, 1 + inner)),
            dma((n, 2)), dma((per, 2)), dma((n, mp)), dma((2, mp)),
            dma((n,)), dma((n,)), dma((3,)),
        ],
        compiler_params=pltpu.CompilerParams(
            collective_id=tag, has_side_effects=True, vmem_limit_bytes=60 * 1024 * 1024
        ),
    )(rows, acts, place, w_out)


def spread(counts, before, base, size):
    r = jnp.arange(size, dtype=jnp.int32)
    inside = (r >= before[..., None]) & (r < (before + counts)[..., None])
    return jnp.sum(jnp.where(inside, (base - before)[..., None] + r + 1, 0), axis=-2) - 1


def local(n, mp, grad_rows, img_start, img_len, img_owner, pre_act, w_out):
    stripe, quarter = grad_rows.shape
    width = pre_act.shape[1]
    kept = w_out.shape[0] // n
    frames = stripe // FRAME
    here = lax.axis_index("seq")
    owner = img_owner.reshape(n, frames)
    starts = img_start.reshape(n, frames)
    lengths = img_len.reshape(n, frames)
    before = jnp.cumsum(lengths, axis=1) - lengths
    row = jnp.arange(FRAME, dtype=jnp.int32)
    column = jnp.arange(stripe, dtype=jnp.int32)

    values = pre_act.astype(jnp.float32)
    activation, derivative = gelu_parts(values)
    activation = activation.astype(jnp.bfloat16)
    acts = activation.reshape(stripe, width // kept, kept).transpose(1, 0, 2)

    my_owner = lax.dynamic_slice_in_dim(owner, here, 1)[0]
    my_start = lax.dynamic_slice_in_dim(starts, here, 1)[0] - here * stripe
    my_length = lax.dynamic_slice_in_dim(lengths, here, 1)[0]
    my_before = lax.dynamic_slice_in_dim(before, here, 1)[0]
    to = (my_owner[None, :] == jnp.arange(n, dtype=jnp.int32)[:, None]).astype(jnp.int32)
    first = jnp.sum(to * my_before[None, :], axis=1)
    count = jnp.sum(to * my_length[None, :], axis=1)
    at = jnp.where(row[None, :] < count[:, None], first[:, None] + row[None, :], -1).reshape(n * FRAME, 1)
    order = img_owner * frames + jnp.arange(n * frames, dtype=jnp.int32) % frames
    factor = 1.0 / math.sqrt(n * stripe)

    def with_size(tag, size, grad_rows, acts, w_out):
        source = spread(my_length, my_before, my_start, size)
        live = (source[:, None] == column[None, :]).astype(jnp.bfloat16)
        rows = jnp.dot(live, grad_rows, preferred_element_type=jnp.float32).astype(jnp.bfloat16)
        place = (at == jnp.arange(size, dtype=jnp.int32)[None, :]).astype(jnp.bfloat16)
        rows_all, act_all, hid = exchange(n, mp, tag, rows, acts, place, w_out)
        blocks = act_all.reshape(n * frames, FRAME, kept)[order].reshape(n, stripe, kept)
        block = jnp.broadcast_to(jnp.arange(frames, dtype=jnp.int32) * FRAME, (n, frames))
        taken = spread(lengths, before, block, size)
        lined = (taken[:, :, None] == column[None, None, :]).astype(jnp.bfloat16)
        act_rows = jnp.einsum(
            "trc,tck->trk", lined, blocks, preferred_element_type=jnp.float32
        ).astype(jnp.bfloat16).reshape(n * size, kept)
        product = lax.dot_general(
            act_rows, rows_all, (((0,), (0,)), ((), ())), preferred_element_type=jnp.float32
        ) * factor
        return lax.optimization_barrier(product.astype(jnp.bfloat16)), hid

    sizes = [stripe // 16 * k for k in (12, 13, 16)]
    most = jnp.max(jnp.sum(lengths, axis=1))
    which = sum((most > size).astype(jnp.int32) for size in sizes[:-1])
    weight_grad, hid = lax.switch(
        which,
        [functools.partial(with_size, tag, size) for tag, size in enumerate(sizes)],
        grad_rows, acts, w_out,
    )

    came = jnp.arange(n * FRAME, dtype=jnp.int32)
    from_me = (owner == here).T
    pick = jnp.repeat(jnp.repeat(from_me, FRAME, axis=0), FRAME, axis=1)
    pick = (pick & (column[:, None] % FRAME == came[None, :] % FRAME)).astype(jnp.bfloat16)
    hidden_grad = jnp.dot(pick, hid, preferred_element_type=jnp.float32)
    pre_grad = (hidden_grad * derivative).astype(jnp.bfloat16)
    return (pre_grad, weight_grad)


def fused_kernel(
    n, mp, inner, size, pieces, early, factor,
    start_ref, len_ref, owner_ref, rows_ref, act_ref, w_ref,
    hid_out, grad_out,
    rows_all, act_all, relay, w_all, acc, hot, block, lined, placed, picked, terms, parts, hid, stage,
    w_sem, rs_recv, rs_send, row_recv, row_send, act_recv, act_send, act_fwd, act_own,
    relay_recv, relay_send, relay_fwd, far_recv, far_send, local_sem, out_sem, before_ref, source_ref,
):
    s = lax.axis_index("seq")
    m = lax.axis_index("mp")
    outer = n // inner
    low = outer // 2
    z, xi = s // inner, s % inner
    piece = size // pieces
    frames = act_ref.shape[0]
    kept = act_all.shape[2]
    per = act_ref.shape[2] // kept
    tokens = frames * FRAME
    half = frames // 2
    quarter = rows_ref.shape[1]
    width = parts.shape[1]
    pair = inner * FRAME
    edge = (z == 0) | (z == outer - 1)
    sibling = m + 1 - 2 * (m % 2)
    opposite = (m + mp // 2) % mp
    seq_peers = [((s + q) % n, m) for q in range(1, n)]
    mp_peers = [(s, (m + q) % mp) for q in range(1, mp)]
    greeted = seq_peers + mp_peers
    barrier = pltpu.get_barrier_semaphore()
    for peer in greeted:
        pl.semaphore_signal(barrier, inc=1, device_id=peer, device_id_type=MESH)

    def remote(src, dst, send, recv, peer):
        return pltpu.make_async_remote_copy(
            src_ref=src, dst_ref=dst, send_sem=send, recv_sem=recv,
            device_id=peer, device_id_type=MESH,
        )

    def go(run, copy):
        if run:
            copy.start()
        else:
            copy.wait_send()

    def loop(first, last, body):
        def step(p, carry):
            body(p)
            return carry
        lax.fori_loop(first, last, step, 0)

    def layer_of(k):
        mate = jnp.where(z < low, low - 1 - z, 3 * low - 1 - z)
        return jnp.where(k == 0, z, jnp.where(k == 1, mate, jnp.where(z < low, k, outer - 1 - k)))

    def row_copy(t, p, way, peer):
        slot = rows_all.at[t // inner, pl.ds((t % inner) * size + p * piece, piece)]
        return remote(slot, slot, row_send.at[t, p, way], row_recv.at[t, p], peer)

    def arrive(run, t, p):
        if run:
            row_copy(t, p, 0, ((s + 1) % n, m)).wait_recv()

    def up(run, t, p):
        @pl.when(z < outer - 1)
        def _():
            go(run, row_copy(t, p, 0, (s + inner, m)))

    def down(run, t, p):
        @pl.when(z > 0)
        def _():
            go(run, row_copy(t, p, 1, (s - inner, m)))

    def across(run, t, p):
        go(run, row_copy(t, p, 2, (z * inner + 1 - xi, m)))

    def own_rows(run, first, last):
        def body(p):
            up(run, s, p)
            down(run, s, p)
            across(run, s, p)
        loop(first, last, body)

    def partner_row(run, p):
        t = z * inner + (1 - xi)
        arrive(run, t, p)
        up(run, t, p)
        down(run, t, p)

    def hop(run, d, first, last):
        def one(p):
            @pl.when(edge & (d == 1) & (p >= early))
            def _():
                partner_row(run, p)

            @pl.when(z >= d)
            def _():
                t = s - d * inner
                arrive(run, t, p)
                up(run, t, p)

                @pl.when((p >= early) & ((d > 1) | (z > 1)))
                def _():
                    across(run, t, p)

                @pl.when(p < early)
                def _():
                    t2 = (z - d) * inner + (1 - xi)
                    arrive(run, t2, p)
                    up(run, t2, p)

            @pl.when(z + d < outer)
            def _():
                t = s + d * inner
                arrive(run, t, p)
                down(run, t, p)

                @pl.when((p >= early) & ((d > 1) | (z < outer - 2)))
                def _():
                    across(run, t, p)

                @pl.when(p < early)
                def _():
                    t2 = (z + d) * inner + (1 - xi)
                    arrive(run, t2, p)
                    down(run, t2, p)
        loop(first, last, one)

    def rest(k):
        t = layer_of(k) * inner + (1 - xi)

        @pl.when((k > 0) | jnp.logical_not(edge))
        def _():
            loop(early, pieces, lambda p: arrive(True, t, p))

    root_a = s // per
    root_b = (root_a + mp // 2) % mp

    def act_slot(t, h):
        return act_all.at[pl.ds(t * frames + h * half, half)]

    def act_piece(j, h):
        return act_ref.at[pl.ds(h * half, half), :, pl.ds(j * kept, kept)]

    def act_mine():
        return pltpu.make_async_copy(
            act_ref.at[:, :, pl.ds(pl.multiple_of(xi * kept, 128), kept)],
            act_all.at[pl.ds(s * frames, frames)], local_sem.at[1],
        )

    def act_first(run):
        for j in range(per):
            target = m * per + j

            @pl.when(target != s)
            def _():
                go(run, remote(
                    act_piece(j, 1), relay.at[j], relay_send.at[j], relay_recv.at[j], (s, opposite)
                ))
                go(run, remote(
                    act_piece(j, 0), act_slot(s, 0), act_send.at[j], act_recv.at[s, 0], (target, m)
                ))

            @pl.when(target == s)
            def _():
                for h in range(2):
                    for q, to in enumerate((opposite, sibling)):
                        go(run, remote(
                            act_piece(j, h), act_slot(s, h), act_own.at[h, q], act_recv.at[s, h], (s, to)
                        ))
                if run:
                    act_mine().start()

    def act_relay(run):
        for j in range(per):
            target = opposite * per + j

            @pl.when(target != s)
            def _():
                if run:
                    remote(
                        relay.at[j], relay.at[j], relay_send.at[j], relay_recv.at[j], (s, opposite)
                    ).wait_recv()
                go(run, remote(
                    relay.at[j], act_slot(s, 1), relay_fwd.at[j], act_recv.at[s, 1], (target, m)
                ))

    def act_wait(t, h):
        remote(act_slot(t, h), act_slot(t, h), act_fwd.at[0, 0, 0], act_recv.at[t, h], mp_peers[0]).wait_recv()

    def act_send_on(run, t, h, to, q):
        go(run, remote(
            act_slot(t, h), act_slot(t, h), act_fwd.at[t, h, q], act_recv.at[t, h], (s, to)
        ))

    def act_pass(run, again):
        def others(body):
            def step(i):
                t = layer_of(i // inner) * inner + i % inner

                @pl.when(t != s)
                def _():
                    body(t)
            loop(0, n, step)

        for h, root in ((0, root_a), (1, root_b)):
            @pl.when(m == root)
            def _():
                def first(t):
                    if run:
                        act_wait(t, h)
                    act_send_on(run, t, h, opposite, 0)
                    act_send_on(run, t, h, sibling, 1)

                def second(t):
                    if run:
                        act_wait(t, 1 - h)
                    act_send_on(run, t, 1 - h, sibling, 1)
                others(second if again else first)

        @pl.when((m == root_b) & again)
        def _():
            for h in range(2):
                if run:
                    act_wait(s, h)
                act_send_on(run, s, h, sibling, 1)

    def act_rest():
        @pl.when((m != root_a) & (m != root_b))
        def _():
            def step(t):
                for h in range(2):
                    act_wait(t, h)
            loop(0, n, step)

        @pl.when(m == root_a)
        def _():
            act_mine().wait()

    def part_copy(run, i, q):
        to = (m + 1 + q) % mp
        go(run, remote(
            terms.at[i % 2, to], parts.at[i * (mp - 1) + mp - 2 - q],
            rs_send.at[i, q], rs_recv.at[i, mp - 2 - q], (s, to),
        ))

    def source(i, j):
        return jnp.where(
            edge,
            jnp.where(i == 0, s, layer_of(jnp.maximum(i - 1, 0)) * inner + j),
            layer_of(i) * inner + j,
        )

    def same(a, b):
        return 1 - jnp.minimum(jnp.abs(a - b), 1)

    def shifted(first, count):
        row = lax.broadcasted_iota(jnp.int32, (FRAME, size), 0)
        column = lax.broadcasted_iota(jnp.int32, (FRAME, size), 1)
        return jnp.where((column - row == first) & (row < count), 1.0, 0.0).astype(jnp.bfloat16)

    def hidden(i):
        @pl.when(i >= 2)
        def _():
            for q in range(mp - 1):
                part_copy(False, i - 2, q)
        tile = 512 if quarter % 512 == 0 else quarter
        for j in range(inner):
            owner = jnp.where(edge & (i == 0), (outer - 1 - z) * inner + j, s)
            first, count = 0, 0
            for f in range(frames):
                at = source(i, j) * frames + f
                hit = same(owner_ref[at], owner)
                first = first + hit * before_ref[at]
                count = count + hit * len_ref[at]
            placed[pl.ds(j * FRAME, FRAME), :] = shifted(first, count)

        def choose(c):
            at = pl.ds(pl.multiple_of(c * tile, tile), tile)
            found = []
            for j in range(inner):
                t = source(i, j)
                rows = rows_all[t // inner, pl.ds(pl.multiple_of((t % inner) * size, 16), size), at]
                found.append(jnp.dot(
                    placed[pl.ds(j * FRAME, FRAME), :], rows, preferred_element_type=jnp.float32,
                ))
            picked[at, :] = jnp.concatenate(found, axis=0).T.astype(jnp.bfloat16)
        loop(0, quarter // tile, choose)

        def step(q):
            to = (m + 1 + q) % mp
            terms[i % 2, to] = jnp.dot(
                w_all[pl.ds(pl.multiple_of(to * width, width), width), :],
                picked[...], preferred_element_type=jnp.float32,
            ).astype(jnp.bfloat16)

            @pl.when(q > 0)
            def _():
                part_copy(True, i, q - 1)
        loop(0, mp, step)

    def reduce(i):
        for q in range(mp - 1):
            at = i * (mp - 1) + q
            remote(
                parts.at[at], parts.at[at], rs_send.at[i, q], rs_recv.at[i, q], mp_peers[q]
            ).wait_recv()
        tile = 256 if width % 256 == 0 else width

        def step(c):
            at = pl.ds(pl.multiple_of(c * tile, tile), tile)
            total = terms[i % 2, m, at, :].astype(jnp.float32)
            for q in range(mp - 1):
                total = total + parts[i * (mp - 1) + q, at, :].astype(jnp.float32)
            total = total.T.astype(jnp.bfloat16)
            for j in range(inner):
                t = jnp.where(edge & (i == 0), n + j, source(i, j))
                hid[t, :, at] = total[j * FRAME:(j + 1) * FRAME]
        loop(0, width // tile, step)

        @pl.when(edge & (i == 0))
        def _():
            far(True)

    def far(run):
        for j in range(inner):
            go(run, remote(
                hid.at[n + j], hid.at[s], far_send.at[j], far_recv.at[xi],
                ((outer - 1 - z) * inner + j, m),
            ))

    def far_wait():
        for j in range(inner):
            t = (outer - 1 - z) * inner + j
            remote(hid.at[t], hid.at[t], far_send.at[j], far_recv.at[j], seq_peers[0]).wait_recv()

    def line_up(k):
        layer = layer_of(k)
        for j in range(inner):
            t = layer * inner + j

            def frame(f):
                at = pl.ds(pl.multiple_of(f * FRAME, FRAME), FRAME)
                i = t * frames + f
                block[at, :] = act_all[jnp.clip(owner_ref[i], 0, n - 1) * frames + f]
                hot[at, :] = shifted(before_ref[i], len_ref[i])
            loop(0, frames, frame)

            def step(c):
                at = pl.ds(pl.multiple_of(c * 128, 128), 128)
                lined[k % 2, at, pl.ds(j * size, size)] = lax.dot_general(
                    block[:, at], hot[...], (((0,), (0,)), ((), ())),
                    preferred_element_type=jnp.float32,
                ).astype(jnp.bfloat16)
            loop(0, kept // 128, step)

    def weights(k):
        layer = layer_of(k)
        tile = stage.shape[2]
        count = quarter // tile

        def put(c, slot):
            at = pl.ds(pl.multiple_of(c * tile, tile), tile)
            return pltpu.make_async_copy(stage.at[slot], grad_out.at[:, at], out_sem.at[slot])

        def step(c):
            at = pl.ds(pl.multiple_of(c * tile, tile), tile)
            value = acc[:, at] + jnp.dot(
                lined[k % 2], rows_all[layer, :, at], preferred_element_type=jnp.float32
            )

            @pl.when(k < outer - 1)
            def _():
                acc[:, at] = value

            @pl.when(k == outer - 1)
            def _():
                slot = c % 2

                @pl.when(c > 1)
                def _():
                    put(c - 2, slot).wait()
                stage[slot] = (value * factor).astype(jnp.bfloat16)
                put(c, slot).start()
        loop(0, count, step)

        @pl.when(k < outer - 1)
        def _():
            line_up(k + 1)

        @pl.when(k == outer - 1)
        def _():
            for c in range(max(0, count - 2), count):
                put(c, c % 2).wait()

    def clear(c):
        at = pl.ds(pl.multiple_of(c * 128, 128), 128)
        acc[at, :] = jnp.zeros((128, quarter), jnp.float32)

    def tables():
        def stripe_sums(t):
            total = 0
            for f in range(frames):
                before_ref[t * frames + f] = total
                total = total + len_ref[t * frames + f]
        loop(0, n, stripe_sums)
        for f in range(frames):
            found = 0
            for t in range(n):
                found = found + same(owner_ref[t * frames + f], s) * t
            source_ref[f] = found

    def gather_map(g):
        row = lax.broadcasted_iota(jnp.int32, (size, 2 * FRAME), 0)
        column = lax.broadcasted_iota(jnp.int32, (size, 2 * FRAME), 1) + g * 2 * FRAME
        hit = None
        for f in range(2):
            at = s * frames + 2 * g + f
            first = before_ref[at]
            shift = start_ref[at] - s * tokens - first
            one = (column - row == shift) & (row >= first) & (row < first + len_ref[at])
            hit = one if hit is None else hit | one
        lined[0, pl.ds(0, size), pl.ds(pl.multiple_of(g * 2 * FRAME, 2 * FRAME), 2 * FRAME)] = (
            jnp.where(hit, 1.0, 0.0).astype(jnp.bfloat16)
        )

    def compact(start, count):
        tile = 512 if quarter % 512 == 0 else quarter

        def step(c):
            at = pl.ds(pl.multiple_of(c * tile, tile), tile)
            rows_all[z, pl.ds(pl.multiple_of(xi * size + start, 16), count), at] = jnp.dot(
                lined[0, pl.ds(start, count), pl.ds(0, tokens)], w_all[pl.ds(0, tokens), at],
                preferred_element_type=jnp.float32,
            ).astype(jnp.bfloat16)
        loop(0, quarter // tile, step)

    rows_in = pltpu.make_async_copy(rows_ref, w_all.at[pl.ds(0, tokens)], local_sem.at[0])
    fetch = pltpu.make_async_copy(
        w_ref.at[pl.ds(tokens, w_ref.shape[0] - tokens)],
        w_all.at[pl.ds(tokens, w_ref.shape[0] - tokens)], w_sem.at[0],
    )
    fetch_top = pltpu.make_async_copy(
        w_ref.at[pl.ds(0, tokens)], w_all.at[pl.ds(0, tokens)], w_sem.at[1]
    )
    rows_in.start()
    fetch.start()
    tables()
    loop(0, tokens // (2 * FRAME), gather_map)
    pl.semaphore_wait(barrier, len(greeted))
    act_first(True)
    rows_in.wait()
    chunk = 4 * piece
    sent = 0
    for at in range(0, size, chunk):
        compact(at, min(chunk, size - at))
        own_rows(True, sent, at // piece)
        sent = at // piece
        if at == chunk:
            act_relay(True)
    own_rows(True, sent, pieces)
    fetch_top.start()
    loop(0, kept // 128, clear)
    loop(0, early, lambda p: partner_row(True, p))
    act_pass(True, False)
    fetch.wait()
    fetch_top.wait()

    def since(e, *steps):
        total = 0
        for at in steps:
            total = total + jnp.where(e >= at, 1, 0)
        return total

    def either(ends, inside):
        return jnp.where(edge, ends, inside)

    def stage_of(e):
        part = e % 4
        hop(True, 1 + e // 4, part * pieces // 4, (part + 1) * pieces // 4)

        @pl.when(e == 1)
        def _():
            act_pass(True, True)
        terms_from = either(since(e, 1, 4, 7, 10), since(e, 2, 6, 8, 10))
        terms_to = either(since(e, 0, 3, 6, 9), since(e, 1, 5, 7, 9))
        grad_from = either(since(e, 5, 8, 11, 12), since(e, 4, 7, 9, 11))
        grad_to = either(since(e, 4, 7, 10, 11), since(e, 3, 6, 8, 10))
        done_from = either(since(e, 3, 7, 10, 12), since(e, 2, 6, 8, 10))
        done_to = either(since(e, 2, 6, 9, 11), since(e, 1, 5, 7, 9))
        loop(done_from, done_to, rest)
        loop(since(e, 5, 9, 11, 12), since(e, 4, 8, 10, 11), reduce)
        loop(terms_from, terms_to, hidden)

        @pl.when(e == 2)
        def _():
            act_rest()
            line_up(0)
        loop(grad_from, grad_to, weights)

    loop(0, 4 * (outer - 1), stage_of)

    @pl.when(edge)
    def _():
        far_wait()
    for f in range(frames):
        hid_out[pl.ds(f * FRAME, FRAME), :] = hid[jnp.clip(source_ref[f], 0, n - 1)]

    act_first(False)
    act_relay(False)
    own_rows(False, 0, pieces)
    for i in range(outer - 2, outer):
        for q in range(mp - 1):
            part_copy(False, i, q)
    loop(0, early, lambda p: partner_row(False, p))
    loop(1, outer, lambda d: hop(False, d, 0, pieces))
    act_pass(False, False)
    act_pass(False, True)

    @pl.when(edge)
    def _():
        far(False)


def fused(n, mp, grain, early, tag, size, factor, starts, lengths, owners, rows, acts, w_out):
    quarter = rows.shape[1]
    frames = acts.shape[0]
    kept = w_out.shape[0] // n
    per = acts.shape[2] // kept
    width = w_out.shape[0] // mp
    inner = n // 4
    outer = n // inner
    pieces = size // grain
    vm = pl.BlockSpec(memory_space=pltpu.VMEM)
    anywhere = pl.BlockSpec(memory_space=pl.ANY)
    dma = pltpu.SemaphoreType.DMA
    b16 = jnp.bfloat16
    return pl.pallas_call(
        functools.partial(fused_kernel, n, mp, inner, size, pieces, max(1, pieces * early // 12), factor),
        out_shape=(
            jax.ShapeDtypeStruct((frames * FRAME, width), b16),
            jax.ShapeDtypeStruct((kept, quarter), b16),
        ),
        in_specs=[pl.BlockSpec(memory_space=pltpu.SMEM)] * 3 + [anywhere] * 3,
        out_specs=(vm, anywhere),
        scratch_shapes=[
            pltpu.VMEM((outer, inner * size, quarter), b16),
            pltpu.VMEM((n * frames, FRAME, kept), b16),
            pltpu.VMEM((per, frames // 2, FRAME, kept), b16),
            pltpu.VMEM(w_out.shape, b16),
            pltpu.VMEM((kept, quarter), jnp.float32),
            pltpu.VMEM((frames * FRAME, size), b16),
            pltpu.VMEM((frames * FRAME, kept), b16),
            pltpu.VMEM((2, kept, inner * size), b16),
            pltpu.VMEM((inner * FRAME, size), b16),
            pltpu.VMEM((quarter, inner * FRAME), b16),
            pltpu.VMEM((2, mp, width, inner * FRAME), b16),
            pltpu.VMEM((outer * (mp - 1), width, inner * FRAME), b16),
            pltpu.VMEM((n + inner, FRAME, width), b16),
            pltpu.VMEM((2, kept, 512 if quarter % 512 == 0 else quarter), b16),
            dma((2,)), dma((outer, mp)), dma((outer, mp)),
            dma((n, pieces)), dma((n, pieces, 3)),
            dma((n, 2)), dma((per,)), dma((n, 2, 2)), dma((2, 2)),
            dma((per,)), dma((per,)), dma((per,)), dma((inner,)), dma((inner,)),
            dma((2,)), dma((2,)),
            pltpu.SMEM((n * frames,), jnp.int32), pltpu.SMEM((frames,), jnp.int32),
        ],
        compiler_params=pltpu.CompilerParams(
            collective_id=tag, has_side_effects=True, vmem_limit_bytes=67043328
        ),
    )(starts, lengths, owners, rows, acts, w_out)


GRAIN, EARLY = 32, 1


def local_fused(n, mp, grad_rows, img_start, img_len, img_owner, pre_act, w_out):
    stripe = grad_rows.shape[0]
    frames = stripe // FRAME
    stripe_of = jnp.arange(n * frames, dtype=jnp.int32) // frames
    inside = stripe_of[None, :] == jnp.arange(n, dtype=jnp.int32)[:, None]
    most = jnp.max(jnp.sum(jnp.where(inside, img_len[None, :], 0), axis=1))
    factor = 1.0 / math.sqrt(n * stripe)
    activation, derivative = gelu_parts(pre_act.astype(jnp.float32))
    acts = activation.astype(jnp.bfloat16).reshape(frames, FRAME, -1)

    def with_size(tag, size, *operands):
        return fused(n, mp, GRAIN, EARLY, tag, size, factor, *operands)

    sizes = [stripe // 16 * k for k in (11, 12, 13, 14, 16)]
    which = sum((most > size).astype(jnp.int32) for size in sizes[:-1])
    hid, weight_grad = lax.switch(
        which,
        [functools.partial(with_size, tag, size) for tag, size in enumerate(sizes)],
        img_start, img_len, img_owner, grad_rows, acts, w_out,
    )
    pre_grad = (hid.astype(jnp.float32) * derivative).astype(jnp.bfloat16)
    return (pre_grad, weight_grad)


def chosen(n, mp, grad_rows, *rest):
    whole = n * grad_rows.shape[0] * grad_rows.shape[1] + rest[-1].shape[0] * rest[-1].shape[1]
    fits = n * FRAME == grad_rows.shape[0] and n == 2 * mp and 2 * whole <= 40 * 1024 * 1024
    return (local_fused if fits else local)(n, mp, grad_rows, *rest)


def solution(mesh):
    return jax.shard_map(
        functools.partial(chosen, mesh.shape["seq"], mesh.shape["mp"]),
        mesh=mesh,
        in_specs=(P("seq", "mp"), P(), P(), P(), P("seq", "mp"), P(None, "mp")),
        out_specs=(P("seq", "mp"), P("seq", "mp")),
        check_vma=False,
    )
```

```python
import functools
import math

import jax
import jax.numpy as jnp
from jax import lax
from jax.experimental import pallas as pl
from jax.experimental.pallas import tpu as pltpu
from jax.sharding import PartitionSpec as P

FRAME = 64
MESH = pl.DeviceIdType.MESH


def gelu_parts(values):
    normal_cdf = 0.5 * (1.0 + lax.erf(values * 0.7071067811865476))
    density = jnp.exp(-0.5 * values * values) * 0.3989422804014327
    return (values * normal_cdf, normal_cdf + values * density)


def exchange_kernel(
    n, mp, inner, pieces,
    rows_ref, act_ref, place_ref, w_ref,
    rows_out, act_out, hid_out,
    terms_ref, parts, outbuf, w_buf, w_sem,
    rs_recv, rs_send, row_recv, row_send, act_recv, act_send, act_fwd, act_own,
    hid_recv, hid_send, local_sem,
):
    s = lax.axis_index("seq")
    m = lax.axis_index("mp")
    outer = n // inner
    z, xi = s // inner, s % inner
    stripe = rows_ref.shape[0]
    piece = stripe // pieces
    tokens = act_ref.shape[1]
    half = tokens // 2
    per = act_ref.shape[0]
    xfirst = inner == 2
    seq_peers = [((s + q) % n, m) for q in range(1, n)]
    mp_peers = [(s, (m + q) % mp) for q in range(1, mp)]

    opposite = (m + mp // 2) % mp
    greeted = seq_peers + mp_peers + [((s + q) % n, opposite) for q in range(1, n)]
    barrier = pltpu.get_barrier_semaphore()
    for peer in greeted:
        pl.semaphore_signal(barrier, inc=1, device_id=peer, device_id_type=MESH)
    pl.semaphore_wait(barrier, len(greeted))

    def remote(src, dst, send, recv, peer):
        return pltpu.make_async_remote_copy(
            src_ref=src, dst_ref=dst, send_sem=send, recv_sem=recv,
            device_id=peer, device_id_type=MESH,
        )

    def row_copy(t, p, way, peer, own=False):
        slot = rows_out.at[pl.ds(t * stripe + p * piece, piece)]
        src = rows_ref.at[pl.ds(p * piece, piece)] if own else slot
        return remote(src, slot, row_send.at[t, p, way], row_recv.at[t, p], peer)

    def go(run, copy):
        if run:
            copy.start()
        else:
            copy.wait_send()

    def arrive(run, t, p):
        if run:
            row_copy(t, p, 0, ((s + 1) % n, m)).wait_recv()

    def up(run, t, p, own=False):
        @pl.when(z < outer - 1)
        def _():
            go(run, row_copy(t, p, 0, (s + inner, m), own))

    def down(run, t, p, own=False):
        @pl.when(z > 0)
        def _():
            go(run, row_copy(t, p, 1, (s - inner, m), own))

    def across(run, t, p, own=False):
        for q in range(1, inner):
            go(run, row_copy(t, p, 1 + q, (z * inner + (xi + q) % inner, m), own))

    def loop(first, body):
        def step(p, carry):
            body(p)
            return carry
        lax.fori_loop(first, pieces, step, 0)

    def own_rows(run):
        def body(p):
            up(run, s, p, True)
            down(run, s, p, True)
            across(run, s, p, True)
        loop(0, body)

    def partner_rows(run):
        if xfirst:
            t = z * inner + (1 - xi)
            for p in range(2):
                arrive(run, t, p)
                up(run, t, p)
                down(run, t, p)

    def hop(run, d):
        def one(p, crossing):
            @pl.when(z >= d)
            def _():
                t = s - d * inner
                arrive(run, t, p)
                up(run, t, p)
                if crossing:
                    across(run, t, p)
                else:
                    t2 = (z - d) * inner + (1 - xi)
                    arrive(run, t2, p)
                    up(run, t2, p)

            @pl.when(z + d < outer)
            def _():
                t = s + d * inner
                arrive(run, t, p)
                down(run, t, p)
                if crossing:
                    across(run, t, p)
                else:
                    t2 = (z + d) * inner + (1 - xi)
                    arrive(run, t2, p)
                    down(run, t2, p)

        if xfirst:
            one(0, False)
            one(1, False)
            loop(2, lambda p: one(p, True))
        else:
            loop(0, lambda p: one(p, True))

    def rest_rows():
        for zz in range(outer):
            for q in range(1, inner):
                t = zz * inner + (xi + q) % inner
                loop(2 if xfirst else 0, lambda p: arrive(True, t, p))

    root_a = s // per
    root_b = (root_a + mp // 2) % mp

    def act_slot(t, h):
        return act_out.at[pl.ds(t * tokens + h * half, half)]

    def act_first(run):
        for j in range(per):
            target = m * per + j

            @pl.when(target != s)
            def _():
                for h, to in ((0, m), (1, opposite)):
                    go(run, remote(
                        act_ref.at[j, pl.ds(h * half, half)], act_slot(s, h),
                        act_send.at[j, h], act_recv.at[s, h], (target, to),
                    ))

            @pl.when(target == s)
            def _():
                for h in range(2):
                    for q, peer in enumerate(mp_peers):
                        go(run, remote(
                            act_ref.at[j, pl.ds(h * half, half)], act_slot(s, h),
                            act_own.at[h, q], act_recv.at[s, h], peer,
                        ))
                mine = pltpu.make_async_copy(
                    act_ref.at[j], act_out.at[pl.ds(s * tokens, tokens)], local_sem.at[1]
                )
                if run:
                    mine.start()
                else:
                    mine.wait()

    def act_wait(t, h):
        remote(act_slot(t, h), act_slot(t, h), act_fwd.at[0, 0], act_recv.at[t, h], mp_peers[0]).wait_recv()

    def act_pass(run):
        for h, root in ((0, root_a), (1, root_b)):
            @pl.when(m == root)
            def _():
                for k in range(1, n):
                    t = (s + k) % n
                    if run:
                        act_wait(t, h)
                    for q, peer in enumerate(mp_peers):
                        go(run, remote(
                            act_slot(t, h), act_slot(t, h), act_fwd.at[t, q], act_recv.at[t, h], peer,
                        ))

    def act_rest():
        for h, root in ((0, root_a), (1, root_b)):
            @pl.when(m != root)
            def _():
                for k in range(1, n):
                    act_wait((s + k) % n, h)

            @pl.when(m != root_a)
            def _():
                act_wait(s, h)

    def sums(run):
        for q, peer in enumerate(mp_peers):
            go(run, remote(terms_ref.at[peer[1]], parts.at[m], rs_send.at[q], rs_recv.at[m], peer))

    def hid_copy(q):
        peer = ((s + q) % n, m)
        return remote(
            outbuf.at[pl.ds(pl.multiple_of(peer[0] * FRAME, FRAME), FRAME)],
            hid_out.at[pl.ds(pl.multiple_of(s * FRAME, FRAME), FRAME)],
            hid_send.at[q], hid_recv.at[s], peer,
        )

    def hid_mine():
        at = pl.ds(pl.multiple_of(s * FRAME, FRAME), FRAME)
        return pltpu.make_async_copy(outbuf.at[at], hid_out.at[at], local_sem.at[2])

    def hidden():
        for q, peer in enumerate(mp_peers):
            remote(terms_ref.at[0], parts.at[peer[1]], rs_send.at[q], rs_recv.at[peer[1]], peer).wait_recv()
        width = parts.shape[2]
        chunk = 256 if width % 256 == 0 else width

        def step(c, carry):
            at = pl.ds(pl.multiple_of(c * chunk, chunk), chunk)
            total = terms_ref[m, :, at].astype(jnp.float32)
            for q in range(1, mp):
                total = total + parts[(m + q) % mp, :, at].astype(jnp.float32)
            outbuf[:, at] = jnp.dot(
                place_ref[...], total.astype(jnp.bfloat16), preferred_element_type=jnp.float32
            ).astype(jnp.bfloat16)
            return carry

        lax.fori_loop(0, width // chunk, step, 0)

    def hid_wait(t):
        at = pl.ds(pl.multiple_of(t * FRAME, FRAME), FRAME)
        remote(outbuf.at[pl.ds(0, FRAME)], hid_out.at[at], hid_send.at[1], hid_recv.at[t], seq_peers[0]).wait_recv()

    def multiply():
        width = terms_ref.shape[2]
        tile = w_buf.shape[1]
        per_part = width // tile

        def where(c):
            return (m + 1 + c // per_part) % mp, (c % per_part) * tile

        def fetch(c, slot):
            q, col = where(c)
            at = pl.ds(pl.multiple_of(q * width + col, tile), tile)
            return pltpu.make_async_copy(w_ref.at[at], w_buf.at[slot], w_sem.at[slot])

        count = mp * per_part
        fetch(0, 0).start()

        def step(c, carry):
            slot = c % 2

            @pl.when(c + 1 < count)
            def _():
                fetch(c + 1, 1 - slot).start()
            fetch(c, slot).wait()
            q, col = where(c)
            terms_ref[q, :, pl.ds(pl.multiple_of(col, tile), tile)] = lax.dot_general(
                rows_ref[...], w_buf[slot], (((1,), (1,)), ((), ())),
                preferred_element_type=jnp.float32,
            ).astype(jnp.bfloat16)
            return carry

        lax.fori_loop(0, count, step, 0)

    keep = pltpu.make_async_copy(rows_ref, rows_out.at[pl.ds(s * stripe, stripe)], local_sem.at[0])
    act_first(True)
    own_rows(True)
    keep.start()
    partner_rows(True)
    multiply()
    sums(True)
    hop(True, 1)
    act_pass(True)
    hidden()
    hop(True, 2)
    for q in range(1, n):
        hid_copy(q).start()
    hid_mine().start()
    for d in range(3, outer):
        hop(True, d)
    rest_rows()
    act_rest()
    for q in range(1, n):
        hid_wait((s + q) % n)

    keep.wait()
    hid_mine().wait()
    own_rows(False)
    sums(False)
    act_first(False)
    partner_rows(False)
    for d in range(1, outer):
        hop(False, d)
    act_pass(False)
    for q in range(1, n):
        hid_copy(q).wait_send()


def exchange(n, mp, tag, rows, acts, place, w_out):
    stripe, quarter = rows.shape
    per, tokens, kept = acts.shape
    width = w_out.shape[0] // mp
    inner = n // 4
    pieces = stripe // 32 if inner == 2 else 1
    vm = pl.BlockSpec(memory_space=pltpu.VMEM)
    anywhere = pl.BlockSpec(memory_space=pl.ANY)
    dma = pltpu.SemaphoreType.DMA
    return pl.pallas_call(
        functools.partial(exchange_kernel, n, mp, inner, pieces),
        out_shape=(
            jax.ShapeDtypeStruct((n * stripe, quarter), jnp.bfloat16),
            jax.ShapeDtypeStruct((n * tokens, kept), jnp.bfloat16),
            jax.ShapeDtypeStruct((n * FRAME, width), jnp.bfloat16),
        ),
        in_specs=[vm] * 3 + [anywhere],
        out_specs=(anywhere,) * 3,
        scratch_shapes=[
            pltpu.VMEM((mp, stripe, width), jnp.bfloat16),
            pltpu.VMEM((mp, stripe, width), jnp.bfloat16),
            pltpu.VMEM((n * FRAME, width), jnp.bfloat16),
            pltpu.VMEM((2, 256 if width % 256 == 0 else width, quarter), jnp.bfloat16),
            dma((2,)),
            dma((mp,)), dma((mp,)),
            dma((n, pieces)), dma((n, pieces, 1 + inner)),
            dma((n, 2)), dma((per, 2)), dma((n, mp)), dma((2, mp)),
            dma((n,)), dma((n,)), dma((3,)),
        ],
        compiler_params=pltpu.CompilerParams(
            collective_id=tag, has_side_effects=True, vmem_limit_bytes=60 * 1024 * 1024
        ),
    )(rows, acts, place, w_out)


def spread(counts, before, base, size):
    r = jnp.arange(size, dtype=jnp.int32)
    inside = (r >= before[..., None]) & (r < (before + counts)[..., None])
    return jnp.sum(jnp.where(inside, (base - before)[..., None] + r + 1, 0), axis=-2) - 1


def local(n, mp, grad_rows, img_start, img_len, img_owner, pre_act, w_out):
    stripe, quarter = grad_rows.shape
    width = pre_act.shape[1]
    kept = w_out.shape[0] // n
    frames = stripe // FRAME
    here = lax.axis_index("seq")
    owner = img_owner.reshape(n, frames)
    starts = img_start.reshape(n, frames)
    lengths = img_len.reshape(n, frames)
    before = jnp.cumsum(lengths, axis=1) - lengths
    row = jnp.arange(FRAME, dtype=jnp.int32)
    column = jnp.arange(stripe, dtype=jnp.int32)

    values = pre_act.astype(jnp.float32)
    activation, derivative = gelu_parts(values)
    activation = activation.astype(jnp.bfloat16)
    acts = activation.reshape(stripe, width // kept, kept).transpose(1, 0, 2)

    my_owner = lax.dynamic_slice_in_dim(owner, here, 1)[0]
    my_start = lax.dynamic_slice_in_dim(starts, here, 1)[0] - here * stripe
    my_length = lax.dynamic_slice_in_dim(lengths, here, 1)[0]
    my_before = lax.dynamic_slice_in_dim(before, here, 1)[0]
    to = (my_owner[None, :] == jnp.arange(n, dtype=jnp.int32)[:, None]).astype(jnp.int32)
    first = jnp.sum(to * my_before[None, :], axis=1)
    count = jnp.sum(to * my_length[None, :], axis=1)
    at = jnp.where(row[None, :] < count[:, None], first[:, None] + row[None, :], -1).reshape(n * FRAME, 1)
    order = img_owner * frames + jnp.arange(n * frames, dtype=jnp.int32) % frames
    factor = 1.0 / math.sqrt(n * stripe)

    def with_size(tag, size, grad_rows, acts, w_out):
        source = spread(my_length, my_before, my_start, size)
        live = (source[:, None] == column[None, :]).astype(jnp.bfloat16)
        rows = jnp.dot(live, grad_rows, preferred_element_type=jnp.float32).astype(jnp.bfloat16)
        place = (at == jnp.arange(size, dtype=jnp.int32)[None, :]).astype(jnp.bfloat16)
        rows_all, act_all, hid = exchange(n, mp, tag, rows, acts, place, w_out)
        blocks = act_all.reshape(n * frames, FRAME, kept)[order].reshape(n, stripe, kept)
        block = jnp.broadcast_to(jnp.arange(frames, dtype=jnp.int32) * FRAME, (n, frames))
        taken = spread(lengths, before, block, size)
        lined = (taken[:, :, None] == column[None, None, :]).astype(jnp.bfloat16)
        act_rows = jnp.einsum(
            "trc,tck->trk", lined, blocks, preferred_element_type=jnp.float32
        ).astype(jnp.bfloat16).reshape(n * size, kept)
        product = lax.dot_general(
            act_rows, rows_all, (((0,), (0,)), ((), ())), preferred_element_type=jnp.float32
        ) * factor
        return lax.optimization_barrier(product.astype(jnp.bfloat16)), hid

    sizes = [stripe // 16 * k for k in (12, 13, 16)]
    most = jnp.max(jnp.sum(lengths, axis=1))
    which = sum((most > size).astype(jnp.int32) for size in sizes[:-1])
    weight_grad, hid = lax.switch(
        which,
        [functools.partial(with_size, tag, size) for tag, size in enumerate(sizes)],
        grad_rows, acts, w_out,
    )

    came = jnp.arange(n * FRAME, dtype=jnp.int32)
    from_me = (owner == here).T
    pick = jnp.repeat(jnp.repeat(from_me, FRAME, axis=0), FRAME, axis=1)
    pick = (pick & (column[:, None] % FRAME == came[None, :] % FRAME)).astype(jnp.bfloat16)
    hidden_grad = jnp.dot(pick, hid, preferred_element_type=jnp.float32)
    pre_grad = (hidden_grad * derivative).astype(jnp.bfloat16)
    return (pre_grad, weight_grad)


def fused_kernel(
    n, mp, inner, size, pieces, early, factor,
    start_ref, len_ref, owner_ref, rows_ref, act_ref, pre_ref, w_ref,
    hid_out, grad_out,
    rows_all, act_all, relay, w_all, acc, hot, block, lined, placed, picked, terms, parts, hid, stage,
    w_sem, rs_recv, rs_send, row_recv, row_send, act_recv, act_send, act_fwd, act_own,
    relay_recv, relay_send, relay_fwd, far_recv, far_send, local_sem, out_sem, before_ref, source_ref,
):
    s = lax.axis_index("seq")
    m = lax.axis_index("mp")
    outer = n // inner
    low = outer // 2
    z, xi = s // inner, s % inner
    piece = size // pieces
    frames = act_ref.shape[0]
    kept = act_all.shape[2]
    per = act_ref.shape[2] // kept
    tokens = frames * FRAME
    half = frames // 2
    quarter = rows_ref.shape[1]
    width = parts.shape[1]
    pair = inner * FRAME
    edge = (z == 0) | (z == outer - 1)
    sibling = m + 1 - 2 * (m % 2)
    opposite = (m + mp // 2) % mp
    seq_peers = [((s + q) % n, m) for q in range(1, n)]
    mp_peers = [(s, (m + q) % mp) for q in range(1, mp)]
    greeted = seq_peers + mp_peers
    barrier = pltpu.get_barrier_semaphore()
    for peer in greeted:
        pl.semaphore_signal(barrier, inc=1, device_id=peer, device_id_type=MESH)

    def remote(src, dst, send, recv, peer):
        return pltpu.make_async_remote_copy(
            src_ref=src, dst_ref=dst, send_sem=send, recv_sem=recv,
            device_id=peer, device_id_type=MESH,
        )

    def go(run, copy):
        if run:
            copy.start()
        else:
            copy.wait_send()

    def loop(first, last, body):
        def step(p, carry):
            body(p)
            return carry
        lax.fori_loop(first, last, step, 0)

    def layer_of(k):
        mate = jnp.where(z < low, low - 1 - z, 3 * low - 1 - z)
        return jnp.where(k == 0, z, jnp.where(k == 1, mate, jnp.where(z < low, k, outer - 1 - k)))

    def row_copy(t, p, way, peer):
        slot = rows_all.at[t // inner, pl.ds((t % inner) * size + p * piece, piece)]
        return remote(slot, slot, row_send.at[t, p, way], row_recv.at[t, p], peer)

    def arrive(run, t, p):
        if run:
            row_copy(t, p, 0, ((s + 1) % n, m)).wait_recv()

    def up(run, t, p):
        @pl.when(z < outer - 1)
        def _():
            go(run, row_copy(t, p, 0, (s + inner, m)))

    def down(run, t, p):
        @pl.when(z > 0)
        def _():
            go(run, row_copy(t, p, 1, (s - inner, m)))

    def across(run, t, p):
        go(run, row_copy(t, p, 2, (z * inner + 1 - xi, m)))

    def own_rows(run, first, last):
        def body(p):
            up(run, s, p)
            down(run, s, p)
            across(run, s, p)
        loop(first, last, body)

    def partner_row(run, p):
        t = z * inner + (1 - xi)
        arrive(run, t, p)
        up(run, t, p)
        down(run, t, p)

    def hop(run, d, first, last):
        def one(p):
            @pl.when(edge & (d == 1) & (p >= early))
            def _():
                partner_row(run, p)

            @pl.when(z >= d)
            def _():
                t = s - d * inner
                arrive(run, t, p)
                up(run, t, p)

                @pl.when((p >= early) & ((d > 1) | (z > 1)))
                def _():
                    across(run, t, p)

                @pl.when(p < early)
                def _():
                    t2 = (z - d) * inner + (1 - xi)
                    arrive(run, t2, p)
                    up(run, t2, p)

            @pl.when(z + d < outer)
            def _():
                t = s + d * inner
                arrive(run, t, p)
                down(run, t, p)

                @pl.when((p >= early) & ((d > 1) | (z < outer - 2)))
                def _():
                    across(run, t, p)

                @pl.when(p < early)
                def _():
                    t2 = (z + d) * inner + (1 - xi)
                    arrive(run, t2, p)
                    down(run, t2, p)
        loop(first, last, one)

    def rest(k):
        t = layer_of(k) * inner + (1 - xi)

        @pl.when((k > 0) | jnp.logical_not(edge))
        def _():
            loop(early, pieces, lambda p: arrive(True, t, p))

    root_a = s // per
    root_b = (root_a + mp // 2) % mp

    def act_slot(t, h):
        return act_all.at[pl.ds(t * frames + h * half, half)]

    def act_piece(j, h):
        return act_ref.at[pl.ds(h * half, half), :, pl.ds(j * kept, kept)]

    def act_mine():
        return pltpu.make_async_copy(
            act_ref.at[:, :, pl.ds(pl.multiple_of(xi * kept, 128), kept)],
            act_all.at[pl.ds(s * frames, frames)], local_sem.at[1],
        )

    def act_first(run):
        for j in range(per):
            target = m * per + j

            @pl.when(target != s)
            def _():
                go(run, remote(
                    act_piece(j, 1), relay.at[j], relay_send.at[j], relay_recv.at[j], (s, opposite)
                ))
                go(run, remote(
                    act_piece(j, 0), act_slot(s, 0), act_send.at[j], act_recv.at[s, 0], (target, m)
                ))

            @pl.when(target == s)
            def _():
                for h in range(2):
                    for q, to in enumerate((opposite, sibling)):
                        go(run, remote(
                            act_piece(j, h), act_slot(s, h), act_own.at[h, q], act_recv.at[s, h], (s, to)
                        ))
                if run:
                    act_mine().start()

    def act_relay(run):
        for j in range(per):
            target = opposite * per + j

            @pl.when(target != s)
            def _():
                if run:
                    remote(
                        relay.at[j], relay.at[j], relay_send.at[j], relay_recv.at[j], (s, opposite)
                    ).wait_recv()
                go(run, remote(
                    relay.at[j], act_slot(s, 1), relay_fwd.at[j], act_recv.at[s, 1], (target, m)
                ))

    def act_wait(t, h):
        remote(act_slot(t, h), act_slot(t, h), act_fwd.at[0, 0, 0], act_recv.at[t, h], mp_peers[0]).wait_recv()

    def act_send_on(run, t, h, to, q):
        go(run, remote(
            act_slot(t, h), act_slot(t, h), act_fwd.at[t, h, q], act_recv.at[t, h], (s, to)
        ))

    def act_pass(run, again):
        def others(body):
            def step(i):
                t = layer_of(i // inner) * inner + i % inner

                @pl.when(t != s)
                def _():
                    body(t)
            loop(0, n, step)

        for h, root in ((0, root_a), (1, root_b)):
            @pl.when(m == root)
            def _():
                def first(t):
                    if run:
                        act_wait(t, h)
                    act_send_on(run, t, h, opposite, 0)
                    act_send_on(run, t, h, sibling, 1)

                def second(t):
                    if run:
                        act_wait(t, 1 - h)
                    act_send_on(run, t, 1 - h, sibling, 1)
                others(second if again else first)

        @pl.when((m == root_b) & again)
        def _():
            for h in range(2):
                if run:
                    act_wait(s, h)
                act_send_on(run, s, h, sibling, 1)

    def act_rest():
        @pl.when((m != root_a) & (m != root_b))
        def _():
            def step(t):
                for h in range(2):
                    act_wait(t, h)
            loop(0, n, step)

        @pl.when(m == root_a)
        def _():
            act_mine().wait()

    def part_copy(run, i, q):
        to = (m + 1 + q) % mp
        go(run, remote(
            terms.at[i % 2, to], parts.at[i * (mp - 1) + mp - 2 - q],
            rs_send.at[i, q], rs_recv.at[i, mp - 2 - q], (s, to),
        ))

    def source(i, j):
        return jnp.where(
            edge,
            jnp.where(i == 0, s, layer_of(jnp.maximum(i - 1, 0)) * inner + j),
            layer_of(i) * inner + j,
        )

    def same(a, b):
        return 1 - jnp.minimum(jnp.abs(a - b), 1)

    def shifted(first, count):
        row = lax.broadcasted_iota(jnp.int32, (FRAME, size), 0)
        column = lax.broadcasted_iota(jnp.int32, (FRAME, size), 1)
        return jnp.where((column - row == first) & (row < count), 1.0, 0.0).astype(jnp.bfloat16)

    def hidden(i):
        @pl.when(i >= 2)
        def _():
            for q in range(mp - 1):
                part_copy(False, i - 2, q)
        tile = 512 if quarter % 512 == 0 else quarter
        for j in range(inner):
            owner = jnp.where(edge & (i == 0), (outer - 1 - z) * inner + j, s)
            first, count = 0, 0
            for f in range(frames):
                at = source(i, j) * frames + f
                hit = same(owner_ref[at], owner)
                first = first + hit * before_ref[at]
                count = count + hit * len_ref[at]
            placed[pl.ds(j * FRAME, FRAME), :] = shifted(first, count)

        def choose(c):
            at = pl.ds(pl.multiple_of(c * tile, tile), tile)
            found = []
            for j in range(inner):
                t = source(i, j)
                rows = rows_all[t // inner, pl.ds(pl.multiple_of((t % inner) * size, 16), size), at]
                found.append(jnp.dot(
                    placed[pl.ds(j * FRAME, FRAME), :], rows, preferred_element_type=jnp.float32,
                ))
            picked[at, :] = jnp.concatenate(found, axis=0).T.astype(jnp.bfloat16)
        loop(0, quarter // tile, choose)

        def step(q):
            to = (m + 1 + q) % mp
            terms[i % 2, to] = jnp.dot(
                w_all[pl.ds(pl.multiple_of(to * width, width), width), :],
                picked[...], preferred_element_type=jnp.float32,
            ).astype(jnp.bfloat16)

            @pl.when(q > 0)
            def _():
                part_copy(True, i, q - 1)
        loop(0, mp, step)

    def reduce(i):
        for q in range(mp - 1):
            at = i * (mp - 1) + q
            remote(
                parts.at[at], parts.at[at], rs_send.at[i, q], rs_recv.at[i, q], mp_peers[q]
            ).wait_recv()
        tile = 256 if width % 256 == 0 else width

        def step(c):
            at = pl.ds(pl.multiple_of(c * tile, tile), tile)
            total = terms[i % 2, m, at, :].astype(jnp.float32)
            for q in range(mp - 1):
                total = total + parts[i * (mp - 1) + q, at, :].astype(jnp.float32)
            total = total.T.astype(jnp.bfloat16)
            for j in range(inner):
                t = jnp.where(edge & (i == 0), n + j, source(i, j))
                hid[t, :, at] = total[j * FRAME:(j + 1) * FRAME]
        loop(0, width // tile, step)

        @pl.when(edge & (i == 0))
        def _():
            far(True)

    def far(run):
        for j in range(inner):
            go(run, remote(
                hid.at[n + j], hid.at[s], far_send.at[j], far_recv.at[xi],
                ((outer - 1 - z) * inner + j, m),
            ))

    def far_wait():
        for j in range(inner):
            t = (outer - 1 - z) * inner + j
            remote(hid.at[t], hid.at[t], far_send.at[j], far_recv.at[j], seq_peers[0]).wait_recv()

    def line_up(k):
        layer = layer_of(k)
        for j in range(inner):
            t = layer * inner + j

            def frame(f):
                at = pl.ds(pl.multiple_of(f * FRAME, FRAME), FRAME)
                i = t * frames + f
                block[at, :] = act_all[jnp.clip(owner_ref[i], 0, n - 1) * frames + f]
                hot[at, :] = shifted(before_ref[i], len_ref[i])
            loop(0, frames, frame)

            def step(c):
                at = pl.ds(pl.multiple_of(c * 128, 128), 128)
                lined[k % 2, at, pl.ds(j * size, size)] = lax.dot_general(
                    block[:, at], hot[...], (((0,), (0,)), ((), ())),
                    preferred_element_type=jnp.float32,
                ).astype(jnp.bfloat16)
            loop(0, kept // 128, step)

    def weights(k):
        layer = layer_of(k)
        tile = stage.shape[2]
        count = quarter // tile

        def put(c, slot):
            at = pl.ds(pl.multiple_of(c * tile, tile), tile)
            return pltpu.make_async_copy(stage.at[slot], grad_out.at[:, at], out_sem.at[slot])

        def step(c):
            at = pl.ds(pl.multiple_of(c * tile, tile), tile)
            value = acc[:, at] + jnp.dot(
                lined[k % 2], rows_all[layer, :, at], preferred_element_type=jnp.float32
            )

            @pl.when(k < outer - 1)
            def _():
                acc[:, at] = value

            @pl.when(k == outer - 1)
            def _():
                slot = c % 2

                @pl.when(c > 1)
                def _():
                    put(c - 2, slot).wait()
                stage[slot] = (value * factor).astype(jnp.bfloat16)
                put(c, slot).start()
        loop(0, count, step)

        @pl.when(k < outer - 1)
        def _():
            line_up(k + 1)

        @pl.when(k == outer - 1)
        def _():
            for c in range(max(0, count - 2), count):
                put(c, c % 2).wait()

    def clear(c):
        at = pl.ds(pl.multiple_of(c * 128, 128), 128)
        acc[at, :] = jnp.zeros((128, quarter), jnp.float32)

    def tables():
        def stripe_sums(t):
            total = 0
            for f in range(frames):
                before_ref[t * frames + f] = total
                total = total + len_ref[t * frames + f]
        loop(0, n, stripe_sums)
        for f in range(frames):
            found = 0
            for t in range(n):
                found = found + same(owner_ref[t * frames + f], s) * t
            source_ref[f] = found

    def gather_map(g):
        row = lax.broadcasted_iota(jnp.int32, (size, 2 * FRAME), 0)
        column = lax.broadcasted_iota(jnp.int32, (size, 2 * FRAME), 1) + g * 2 * FRAME
        hit = None
        for f in range(2):
            at = s * frames + 2 * g + f
            first = before_ref[at]
            shift = start_ref[at] - s * tokens - first
            one = (column - row == shift) & (row >= first) & (row < first + len_ref[at])
            hit = one if hit is None else hit | one
        lined[0, pl.ds(0, size), pl.ds(pl.multiple_of(g * 2 * FRAME, 2 * FRAME), 2 * FRAME)] = (
            jnp.where(hit, 1.0, 0.0).astype(jnp.bfloat16)
        )

    def compact(start, count):
        tile = 512 if quarter % 512 == 0 else quarter

        def step(c):
            at = pl.ds(pl.multiple_of(c * tile, tile), tile)
            rows_all[z, pl.ds(pl.multiple_of(xi * size + start, 16), count), at] = jnp.dot(
                lined[0, pl.ds(start, count), pl.ds(0, tokens)], w_all[pl.ds(0, tokens), at],
                preferred_element_type=jnp.float32,
            ).astype(jnp.bfloat16)
        loop(0, quarter // tile, step)

    rows_in = pltpu.make_async_copy(rows_ref, w_all.at[pl.ds(0, tokens)], local_sem.at[0])
    fetch = pltpu.make_async_copy(
        w_ref.at[pl.ds(tokens, w_ref.shape[0] - tokens)],
        w_all.at[pl.ds(tokens, w_ref.shape[0] - tokens)], w_sem.at[0],
    )
    fetch_top = pltpu.make_async_copy(
        w_ref.at[pl.ds(0, tokens)], w_all.at[pl.ds(0, tokens)], w_sem.at[1]
    )
    pre_in = pltpu.make_async_copy(pre_ref, hid_out, w_sem.at[2])
    rows_in.start()
    fetch.start()
    pre_in.start()
    tables()
    loop(0, tokens // (2 * FRAME), gather_map)
    pl.semaphore_wait(barrier, len(greeted))
    act_first(True)
    rows_in.wait()
    chunk = 4 * piece
    sent = 0
    for at in range(0, size, chunk):
        compact(at, min(chunk, size - at))
        own_rows(True, sent, at // piece)
        sent = at // piece
        if at == chunk:
            act_relay(True)
    own_rows(True, sent, pieces)
    fetch_top.start()
    loop(0, kept // 128, clear)
    loop(0, early, lambda p: partner_row(True, p))
    act_pass(True, False)
    fetch.wait()
    fetch_top.wait()

    def since(e, *steps):
        total = 0
        for at in steps:
            total = total + jnp.where(e >= at, 1, 0)
        return total

    def either(ends, inside):
        return jnp.where(edge, ends, inside)

    def derive(f):
        at = pl.ds(pl.multiple_of(f * 16, 16), 16)
        hid_out[at, :] = gelu_parts(hid_out[at, :].astype(jnp.float32))[1].astype(jnp.bfloat16)

    pre_in.wait()
    loop(0, tokens // 16, derive)

    def stage_of(e):
        part = e % 4
        hop(True, 1 + e // 4, part * pieces // 4, (part + 1) * pieces // 4)

        @pl.when(e == 1)
        def _():
            act_pass(True, True)
        terms_from = either(since(e, 1, 4, 7, 10), since(e, 2, 6, 8, 10))
        terms_to = either(since(e, 0, 3, 6, 9), since(e, 1, 5, 7, 9))
        grad_from = either(since(e, 5, 8, 11, 12), since(e, 4, 7, 9, 11))
        grad_to = either(since(e, 4, 7, 10, 11), since(e, 3, 6, 8, 10))
        done_from = either(since(e, 3, 7, 10, 12), since(e, 2, 6, 8, 10))
        done_to = either(since(e, 2, 6, 9, 11), since(e, 1, 5, 7, 9))
        loop(done_from, done_to, rest)
        loop(since(e, 5, 9, 11, 12), since(e, 4, 8, 10, 11), reduce)
        loop(terms_from, terms_to, hidden)

        @pl.when(e == 2)
        def _():
            act_rest()
            line_up(0)
        loop(grad_from, grad_to, weights)

    loop(0, 4 * (outer - 1), stage_of)

    @pl.when(edge)
    def _():
        far_wait()
    for f in range(frames):
        at = pl.ds(f * FRAME, FRAME)
        value = hid[jnp.clip(source_ref[f], 0, n - 1)].astype(jnp.float32)
        hid_out[at, :] = (value * hid_out[at, :].astype(jnp.float32)).astype(jnp.bfloat16)

    act_first(False)
    act_relay(False)
    own_rows(False, 0, pieces)
    for i in range(outer - 2, outer):
        for q in range(mp - 1):
            part_copy(False, i, q)
    loop(0, early, lambda p: partner_row(False, p))
    loop(1, outer, lambda d: hop(False, d, 0, pieces))
    act_pass(False, False)
    act_pass(False, True)

    @pl.when(edge)
    def _():
        far(False)


def fused(n, mp, grain, early, tag, size, factor, starts, lengths, owners, rows, acts, pre_act, w_out):
    quarter = rows.shape[1]
    frames = acts.shape[0]
    kept = w_out.shape[0] // n
    per = acts.shape[2] // kept
    width = w_out.shape[0] // mp
    inner = n // 4
    outer = n // inner
    pieces = size // grain
    vm = pl.BlockSpec(memory_space=pltpu.VMEM)
    anywhere = pl.BlockSpec(memory_space=pl.ANY)
    dma = pltpu.SemaphoreType.DMA
    b16 = jnp.bfloat16
    return pl.pallas_call(
        functools.partial(fused_kernel, n, mp, inner, size, pieces, max(1, pieces * early // 12), factor),
        out_shape=(
            jax.ShapeDtypeStruct((frames * FRAME, width), b16),
            jax.ShapeDtypeStruct((kept, quarter), b16),
        ),
        in_specs=[pl.BlockSpec(memory_space=pltpu.SMEM)] * 3 + [anywhere] * 4,
        out_specs=(vm, anywhere),
        scratch_shapes=[
            pltpu.VMEM((outer, inner * size, quarter), b16),
            pltpu.VMEM((n * frames, FRAME, kept), b16),
            pltpu.VMEM((per, frames // 2, FRAME, kept), b16),
            pltpu.VMEM(w_out.shape, b16),
            pltpu.VMEM((kept, quarter), jnp.float32),
            pltpu.VMEM((frames * FRAME, size), b16),
            pltpu.VMEM((frames * FRAME, kept), b16),
            pltpu.VMEM((2, kept, inner * size), b16),
            pltpu.VMEM((inner * FRAME, size), b16),
            pltpu.VMEM((quarter, inner * FRAME), b16),
            pltpu.VMEM((2, mp, width, inner * FRAME), b16),
            pltpu.VMEM((outer * (mp - 1), width, inner * FRAME), b16),
            pltpu.VMEM((n + inner, FRAME, width), b16),
            pltpu.VMEM((2, kept, 512 if quarter % 512 == 0 else quarter), b16),
            dma((3,)), dma((outer, mp)), dma((outer, mp)),
            dma((n, pieces)), dma((n, pieces, 3)),
            dma((n, 2)), dma((per,)), dma((n, 2, 2)), dma((2, 2)),
            dma((per,)), dma((per,)), dma((per,)), dma((inner,)), dma((inner,)),
            dma((2,)), dma((2,)),
            pltpu.SMEM((n * frames,), jnp.int32), pltpu.SMEM((frames,), jnp.int32),
        ],
        compiler_params=pltpu.CompilerParams(
            collective_id=tag, has_side_effects=True, vmem_limit_bytes=67043328
        ),
    )(starts, lengths, owners, rows, acts, pre_act, w_out)


GRAIN, EARLY = 32, 1


def local_fused(n, mp, grad_rows, img_start, img_len, img_owner, pre_act, w_out):
    stripe = grad_rows.shape[0]
    frames = stripe // FRAME
    stripe_of = jnp.arange(n * frames, dtype=jnp.int32) // frames
    inside = stripe_of[None, :] == jnp.arange(n, dtype=jnp.int32)[:, None]
    totals = jnp.sum(jnp.where(inside, img_len[None, :], 0), axis=1)
    factor = 1.0 / math.sqrt(n * stripe)
    activation, _ = gelu_parts(pre_act.astype(jnp.float32))
    acts = activation.astype(jnp.bfloat16).reshape(frames, FRAME, -1)

    def with_size(tag, size, *operands):
        return fused(n, mp, GRAIN, EARLY, tag, size, factor, *operands)

    sizes = [stripe // 16 * k for k in (11, 12, 13, 14, 16)]
    which = jnp.max(sum((totals > size).astype(jnp.int32) for size in sizes[:-1]))
    return lax.switch(
        which,
        [functools.partial(with_size, tag, size) for tag, size in enumerate(sizes)],
        img_start, img_len, img_owner, grad_rows, acts, pre_act, w_out,
    )


def chosen(n, mp, grad_rows, *rest):
    whole = n * grad_rows.shape[0] * grad_rows.shape[1] + rest[-1].shape[0] * rest[-1].shape[1]
    fits = n * FRAME == grad_rows.shape[0] and n == 2 * mp and 2 * whole <= 40 * 1024 * 1024
    return (local_fused if fits else local)(n, mp, grad_rows, *rest)


def solution(mesh):
    return jax.shard_map(
        functools.partial(chosen, mesh.shape["seq"], mesh.shape["mp"]),
        mesh=mesh,
        in_specs=(P("seq", "mp"), P(), P(), P(), P("seq", "mp"), P(None, "mp")),
        out_specs=(P("seq", "mp"), P("seq", "mp")),
        check_vma=False,
    )
```
